256 devices in a mesh: expert: 8 (over x, core), ffn: 32 (over z, y).
Axes of the slice: x: 4, y: 4, z: 8, core: 2. Of those that a mesh axis runs over, the one named last changes fastest.
Arguments:
- tokens: bfloat16 [8, 128, 4096], P('expert', 'ffn'), may hold values from -6 to 6
- routes: int32 [8, 128, 2], P('expert'), may hold values from 0 to 7, all different within a row; in each aligned block of 128 rows (0 to 127, 128 to 255, ..., all dimensions but the last counted through in order) at most 48 rows name the same one
- router: bfloat16 [4096, 8], replicated, may hold values from -0.09375 to 0.09375
- w_gate: bfloat16 [8, 4096, 12288], P('expert', None, 'ffn'), may hold values from -0.09375 to 0.09375
- w_up: bfloat16 [8, 4096, 12288], P('expert', None, 'ffn'), may hold values from -0.09375 to 0.09375
- w_down: bfloat16 [8, 12288, 4096], P('expert', 'ffn'), may hold values from -0.109375 to 0.109375
- adapter: bfloat16 [8, 4096, 4096], P('expert', None, 'ffn'), may hold values from -0.09375 to 0.09375
- upstream: bfloat16 [8, 128, 4096], P('expert', None, 'ffn'), may hold values from -24 to 24
- bound: float32 [8], P('expert'), may hold values from 2048 to 16384
Outputs:
- adapted: bfloat16 [8, 128, 4096], P('expert', None, 'ffn')
- clipped: bfloat16 [8, 4096, 4096], P('expert', None, 'ffn')
The draws below stay inside these ranges and needn't reach their ends.
Inputs may be any that keep to these rules, and one draw needn't show every extreme that they name: `routes`: each token names two different experts; for each client at most 48 of its tokens name any one expert, and in some clients some expert is named by exactly 48 tokens.
All inputs are finite; a program needn't handle non-finite values.
Results may differ from the reference program's by a relative error of at most 0.015.
Values may be sent and summed in bfloat16 or wider, within the bound.
A program may use at most 64 MiB of HBM per device.

```python
import math
import jax
import jax.numpy as jnp
import numpy as np
from jax import lax

D = 4096
FF = 12288
EXPERTS = 8
CLIENTS = 8
TOK_CL = 128
CAP = 48
FF_DEV = 384
COLS_DEV = 128
N_FFN = 32


def draw_upstream(key, part):
    key_noise = jax.random.fold_in(key, 11)
    key_scale = jax.random.fold_in(key, 23)
    noise_part = jax.random.normal(key_noise, (CLIENTS, TOK_CL, D), jnp.float32)
    block_scales = jnp.exp(jax.random.uniform(key_scale, (CLIENTS, 1, D // COLS_DEV), jnp.float32, math.log(0.25), math.log(4.0)))
    scales = jnp.repeat(block_scales, COLS_DEV, axis=2)
    values = noise_part * scales
    return jnp.clip(values, -24.0, 24.0).astype(jnp.bfloat16)


def raised(array, own_key, source, target, blocks, factor):
    def block_of(position):
        return (jnp.arange(array.shape[position]) // (array.shape[position] // blocks)).reshape((-1,) + (1,) * (array.ndim - 1 - position))

    first = jax.random.permutation(own_key, blocks)[block_of(target)]
    far = (block_of(target) + blocks // 2) % blocks
    return jnp.where((block_of(source) == first) | (block_of(source) == far), factor * array, array)


def shard_levels(key, extent, cuts, smallest, largest):
    loudness = 1.0
    for position, parts in cuts:
        steps = jax.random.uniform(jax.random.fold_in(jax.random.fold_in(key, 6), position), (parts,), jnp.float32, smallest / len(cuts), largest / len(cuts))
        loudness = loudness * jnp.repeat(jnp.exp(steps), extent[position] // parts).reshape((-1,) + (1,) * (len(extent) - 1 - position))
    return loudness


def routed_block(key, own, number, rows, number_of, top, limit, lean):
    sequence = jax.random.permutation(key, number_of)
    crowded, ordinary = shares(number_of, rows * top, limit, lean, True), shares(number_of, rows * top, limit, lean, False)
    places = jnp.arange(number_of)

    def named(tallies, turn):
        used = int((tallies > 0).sum())
        fixed = max(1, used // 4)
        passed = fixed + (places - fixed + turn * (used - fixed)) % max(1, number_of - fixed)
        return jnp.zeros((number_of,), jnp.int32).at[sequence[jnp.where(places < fixed, places, passed)]].set(jnp.asarray(tallies, jnp.int32))

    tallies = jnp.where(number % 4 == 0, named(crowded, number // 4), named(ordinary, number - number // 4 - 1))
    mixed = jax.random.permutation(jax.random.fold_in(own, 3), number_of)
    donor, taker = mixed[0:number_of // 2 * 2:2], mixed[1:number_of // 2 * 2:2]
    slack = jnp.minimum(tallies[donor] - 1, limit - tallies[taker]) // 2
    slack = jnp.where((donor == sequence[0]) | (taker == sequence[0]) | (tallies[taker] == 0), 0, jnp.maximum(slack, 0))
    passed = jax.random.randint(jax.random.fold_in(own, 4), (number_of // 2,), 0, 1 << 20) % (slack + 1)
    tallies = tallies.at[donor].add(-passed).at[taker].add(passed)
    members = jnp.searchsorted(jnp.cumsum(tallies), jnp.arange(rows * top), side="right").astype(jnp.int32)
    grid = members.reshape(top, rows).T
    grid = grid[jax.random.permutation(jax.random.fold_in(own, 1), rows)]
    turn = jax.random.randint(jax.random.fold_in(own, 2), (rows, 1), 0, top)
    return jnp.take_along_axis(grid, (jnp.arange(top)[None, :] + turn) % top, axis=1)


def shares(amount, total, most, skew, full):
    loads = [(1 << 20) // math.isqrt(grade ** skew) + 1 for grade in range(1, amount + 1)]
    largest = most if full else min(most, max(-(-total // amount), total * loads[0] // sum(loads)))
    least = 1 if total - largest >= amount - 1 else 0
    counts, spare = [largest] + [least] * (amount - 1), total - largest - least * (amount - 1)
    while spare > 0:
        candidates = [i for i in range(1, amount) if counts[i] < largest] or [i for i in range(1, amount) if counts[i] < most]
        pool, left = sum([loads[i] for i in candidates]), spare
        for i in candidates:
            more = min(most - counts[i], max(1, left * loads[i] // pool), spare)
            counts[i] = counts[i] + more
            spare = spare - more
    return np.array(counts)


def noise(key, extent, scale, most, shards=(), held_as=jnp.bfloat16):
    array = jax.random.normal(key, extent, jnp.float32) * scale
    if len(shards) > 0:
        array = shard_levels(key, extent, shards, -0.22, 0.18) * array
    return jnp.clip(array, min=-most, max=most).astype(held_as)


def noise_with(key, dims, scale, limit, pieces, heavy, held_as=jnp.bfloat16):
    array = scale * jax.random.normal(key, dims, jnp.float32)
    if pieces:
        array = array * shard_levels(key, dims, pieces, -0.22, 0.18)
    return jnp.clip(raised(array, jax.random.fold_in(key, 3), *heavy), -limit, limit).astype(held_as)


def setup_inputs(seed: int = 0) -> dict:
    key_list = jax.random.split(jax.random.key(seed), 10)
    tokens = noise(key_list[0], (CLIENTS, TOK_CL, D), 1.0, 6.0, ((0, 8), (1, 32)))
    routes_keys = jax.random.split(jax.random.fold_in(key_list[1], 1), CLIENTS * TOK_CL // TOK_CL)
    routes_turns = jax.random.permutation(jax.random.fold_in(key_list[1], 3), CLIENTS * TOK_CL // TOK_CL)
    routes = jax.vmap(lambda own, number: routed_block(jax.random.fold_in(key_list[1], 2), own, number, TOK_CL, EXPERTS, 2, CAP, 1))(routes_keys, routes_turns).reshape((CLIENTS, TOK_CL, 2))
    router = noise(key_list[2], (D, EXPERTS), D ** -0.5, 0.09375)
    w_gate = noise(key_list[3], (EXPERTS, D, FF), D ** -0.5, 0.09375, ((0, 8), (2, 32)))
    w_up = noise(key_list[4], (EXPERTS, D, FF), D ** -0.5, 0.09375, ((0, 8), (2, 32)))
    w_down = noise_with(key_list[5], (EXPERTS, FF, D), FF ** -0.5, 0.109375, ((0, 8), (1, 32)), (1, 2, 32, 2.75))
    adapter = noise(key_list[6], (CLIENTS, D, D), D ** -0.5, 0.09375, ((0, 8), (2, 32)))
    upstream = draw_upstream(jax.random.fold_in(key_list[9], 71), 0)
    bound = jnp.clip(jnp.exp(math.log(16384.0) - 2.0794415 * jax.random.uniform(key_list[8], (CLIENTS,), jnp.float32) ** shard_levels(key_list[8], (CLIENTS,), ((0, 8),), -0.2, 0.2)), 2048.0, 16384.0)
    return {"tokens": tokens, "routes": routes, "router": router, "w_gate": w_gate, "w_up": w_up, "w_down": w_down, "adapter": adapter, "upstream": upstream, "bound": bound}


def slot_table(routed, expert_count):
    named_hits = lax.optimization_barrier(jnp.sum((routed[:, :, None] == jnp.arange(expert_count, dtype=jnp.int32)[None, None, :]).astype(jnp.int32), axis=1))
    before = jnp.cumsum(named_hits, axis=0) - named_hits
    return jnp.take_along_axis(before, routed, axis=1).astype(jnp.int32)

def pack_rows(token_rows, routed, expert_count, capacity):
    token_count = token_rows.shape[0]
    slot_flat = (routed * capacity + slot_table(routed, expert_count)).astype(jnp.int32)
    owners = jnp.repeat(jnp.arange(token_count, dtype=jnp.int32), 2)
    source = jnp.full((expert_count * capacity,), token_count, jnp.int32).at[slot_flat.reshape(-1)].set(owners)
    padded = jnp.concatenate([token_rows, jnp.zeros((1, token_rows.shape[1]), token_rows.dtype)], axis=0)
    return (padded[source].reshape(expert_count, capacity, token_rows.shape[1]), slot_flat)

def mix_weights(token_rows, routed, router):
    logits = jnp.dot(token_rows, router, preferred_element_type=jnp.float32)
    picked = jnp.take_along_axis(logits, routed, axis=1)
    weight_first = jax.nn.sigmoid(picked[:, 0] - picked[:, 1])
    return (weight_first, 1.0 - weight_first)

def reference(tokens, routes, router, w_gate, w_up, w_down, adapter, upstream, bound):

    def pack_one(token_rows, routed):
        return pack_rows(token_rows, routed, EXPERTS, CAP)
    packed, slot_flats = jax.vmap(pack_one)(tokens, routes)

    def add_block(running, operand_pair):
        down_piece = jnp.dot(operand_pair[0], operand_pair[1], preferred_element_type=jnp.float32).astype(jnp.bfloat16)
        down_piece = lax.optimization_barrier(down_piece)
        return (running + down_piece.astype(jnp.float32), None)

    def expert_one(inputs):
        expert_rows, gate_w, up_w, down_w = inputs
        flat_rows = expert_rows.reshape(-1, D)
        gate_out = jnp.dot(flat_rows, gate_w, preferred_element_type=jnp.float32)
        up_out = jnp.dot(flat_rows, up_w, preferred_element_type=jnp.float32)
        hidden = (jax.nn.silu(gate_out) * up_out).astype(jnp.bfloat16)
        blocks = jnp.transpose(hidden.reshape(-1, N_FFN, FF_DEV), (1, 0, 2))
        down_blocks = down_w.reshape(N_FFN, FF_DEV, D)
        running, _ = lax.scan(add_block, jnp.zeros((CLIENTS * CAP, D), jnp.float32), (blocks, down_blocks))
        return running.reshape(CLIENTS, CAP, D)
    expert_out = lax.map(expert_one, (jnp.moveaxis(packed, 1, 0), w_gate, w_up, w_down))
    by_client = jnp.moveaxis(expert_out, 0, 1).reshape(CLIENTS, EXPERTS * CAP, D)

    def client_one(inputs):
        token_rows, routed, slot_flat, expert_rows, adapt_matrix, grad_input, clip_limit = inputs
        weight_first, weight_second = mix_weights(token_rows, routed, router)
        picked = expert_rows[slot_flat]
        mixture = weight_first[:, None] * picked[:, 0] + weight_second[:, None] * picked[:, 1]
        layer_out = (token_rows.astype(jnp.float32) + mixture).astype(jnp.bfloat16)
        adapted = (layer_out.astype(jnp.float32) + jnp.dot(layer_out, adapt_matrix, preferred_element_type=jnp.float32)).astype(jnp.bfloat16)
        adapter_grad = lax.dot_general(layer_out, grad_input, (((0,), (0,)), ((), ())), preferred_element_type=jnp.float32)
        grad_norm = jnp.sqrt(jnp.sum(adapter_grad * adapter_grad))
        factor = clip_limit / jnp.maximum(grad_norm, clip_limit)
        return (adapted, (adapter_grad * factor).astype(jnp.bfloat16))
    adapted, clipped = lax.map(client_one, (tokens, routes, slot_flats, by_client, adapter, upstream, bound))
    return (adapted, clipped)
```

```python
import functools

import jax
import jax.numpy as jnp
from jax import lax
from jax.experimental import pallas as pl
from jax.experimental.pallas import tpu as pltpu
from jax.sharding import PartitionSpec as P

MESH = pl.DeviceIdType.MESH
NZ, NY = 8, 4
CAP = 48
bf16, f32 = jnp.bfloat16, jnp.float32


class Plan:
    def __init__(self, rows, rows_a):
        half_a = -(-rows_a // 32) * 16
        rows_b = rows - rows_a
        half_b = -(-rows_b // 32) * 16
        A = (0, rows_a)
        A1, A2 = (0, half_a), (half_a, rows_a - half_a)
        B = (rows_a, rows_b)
        B1, B2 = (rows_a, half_b), (rows_a + half_b, rows_b - half_b)
        far = NZ // 2
        msgs, deps, gen = {}, {}, {}

        def add(key, step, block, rows, needs):
            msgs[key] = (step, block, rows)
            deps[key] = needs
            gen[key] = 1 + max([gen[n] for n in needs], default=0)

        for k in range(1, far + 1):
            for s in (1, -1):
                rows_k = A if k < far else (A1 if s > 0 else A2)
                add(("Az", s, k), (s, 0), (-s * (k - 1), 0), rows_k,
                    [("Az", s, k - 1)] if k > 1 else [])
        for k in range(1, 3):
            for s in (1, -1):
                rows_k = B if k < 2 else (B1 if s > 0 else B2)
                add(("By", s, k), (0, s), (0, -s * (k - 1)), rows_k,
                    [("By", s, k - 1)] if k > 1 else [])
        for bz in (0, -1, 1, -2, 2, -3, 3, -4):
            if bz == 0:
                needs = []
            elif abs(bz) < far:
                needs = [("Az", 1 if bz < 0 else -1, abs(bz))]
            else:
                needs = [("Az", 1, far), ("Az", -1, far)]
            for k in range(1, 3):
                for s in (1, -1):
                    rows_k = A if k < 2 else (A1 if s > 0 else A2)
                    add(("Ay", bz, s, k), (0, s), (bz, -s * (k - 1)), rows_k,
                        [("Ay", bz, s, k - 1)] if k > 1 else needs)
        for by in (0, -1, 1, 2):
            if by == 0:
                needs = []
            elif abs(by) < 2:
                needs = [("By", 1 if by < 0 else -1, 1)]
            else:
                needs = [("By", 1, 2), ("By", -1, 2)]
            for k in range(1, far + 1):
                for s in (1, -1):
                    rows_k = B if k < far else (B1 if s > 0 else B2)
                    add(("Bz", by, s, k), (s, 0), (-s * (k - 1), by), rows_k,
                        [("Bz", by, s, k - 1)] if k > 1 else needs)
        self.msgs, self.deps, self.gen = msgs, deps, gen
        self.keys = list(msgs)
        self.index = {key: i for i, key in enumerate(self.keys)}
        self.order = sorted(self.keys, key=lambda key: gen[key])
        self.last = max(gen.values())
        self.users = {key: [k2 for k2 in self.keys if key in deps[k2]] for key in self.keys}
        self.offset, total = {}, 0
        for key in self.keys:
            self.offset[key] = total
            total += msgs[key][2][1]
        self.total = total


SLOTS = Plan(8 * CAP, 224)
LAYER = Plan(128, 64)


def layer_kernel(
    tok_ref, routes_ref, router_ref, wg_hbm, wu_hbm, wd_hbm, ad_hbm, up_ref, bound_ref,
    adapted_ref, clipped_ref,
    w, wd, ad, tok_s, tok_y, tok_z, aux_s, aux_y, aux_z, gall, lgp, tcol, pm, whi, wlo,
    pks, buf, acc, hid, vb, rb, rx, lbuf, grad, gram, adp,
    w_sem, a1s, a1r, a2s, a2r, b1s, b1r, b2s, b2r, g1s, g1r, g2s, g2r,
    xs, xr, ys, yr, ags, agr, rss, rsr, lgs, lgr,
):
    E = 8
    D = NZ * NY * 128
    e = lax.axis_index("expert")
    f = lax.axis_index("ffn")
    z, y = f // NY, lax.rem(f, NY)

    loads = []
    for g in range(NZ):
        rows = pl.ds(g * 512, 512)
        loads.append(pltpu.make_async_copy(wg_hbm.at[rows, :], w.at[0, g], w_sem.at[0, g]))
        loads.append(pltpu.make_async_copy(wu_hbm.at[rows, :], w.at[1, g], w_sem.at[1, g]))
    late_loads = []
    for g in range(NZ):
        late_loads.append(pltpu.make_async_copy(
            wd_hbm.at[:, pl.ds(g * 512, 512)], wd.at[g], w_sem.at[2, g]))
        late_loads.append(pltpu.make_async_copy(
            ad_hbm.at[pl.ds(g * 512, 512), :], ad.at[g], w_sem.at[3, g]))

    def at(dz, dy):
        return lax.rem(z + dz + NZ, NZ) * NY + lax.rem(y + dy + NY, NY)

    def ffn(dz, dy):
        return {"ffn": at(dz, dy)}

    def peer(d):
        return {"expert": lax.rem(e + d, E)}

    barrier = pltpu.get_barrier_semaphore()
    for dy in range(1, NY):
        pl.semaphore_signal(barrier, inc=1, device_id=ffn(0, dy), device_id_type=MESH)
    for dz in range(1, NZ):
        pl.semaphore_signal(barrier, inc=1, device_id=ffn(dz, 0), device_id_type=MESH)
    for d in range(1, E):
        pl.semaphore_signal(barrier, inc=1, device_id=peer(d), device_id_type=MESH)

    for load in loads:
        load.start()

    for i in range(NZ * NY):
        tok_s[i % NY, i // NY] = tok_ref[:, i * 128:(i + 1) * 128]
    tok_y[y] = tok_s[y]
    lgp[...] = jnp.zeros_like(lgp)
    lgp[0:4, 0:E] = lax.dot_general(
        tok_ref[...], router_ref[...], (((1,), (1,)), ((), ())), preferred_element_type=f32
    )
    own_logits = lgp[0:4, :]
    own_gram = lax.dot_general(
        up_ref[...], up_ref[...], (((1,), (1,)), ((), ())), preferred_element_type=f32
    )
    for i in range(NZ * NY):
        aux_s[i % NY, i // NY, 0:4, :] = own_logits
        aux_s[i % NY, i // NY, 4:8, :] = own_gram[4 * i:4 * i + 4, :]
    aux_y[y] = aux_s[y]

    first, second = routes_ref[0:1, :], routes_ref[1:2, :]
    expert_ids = lax.broadcasted_iota(jnp.int32, (E, 128), 0)
    hits = ((expert_ids == first) | (expert_ids == second)).astype(f32)
    before = (
        lax.broadcasted_iota(jnp.int32, (128, 128), 0)
        < lax.broadcasted_iota(jnp.int32, (128, 128), 1)
    ).astype(f32)
    rank = jnp.dot(hits.astype(bf16), before.astype(bf16), preferred_element_type=f32)
    slot = jnp.where(hits > 0.0, rank, -1.0)
    slot_ids = lax.broadcasted_iota(jnp.int32, (CAP, 128), 0).astype(f32)
    for i in range(E):
        pm[i * CAP:(i + 1) * CAP, :] = (slot_ids == slot[i:i + 1, :]).astype(f32)

    pl.semaphore_wait(barrier, NY - 1 + NZ - 1 + E - 1)

    sent = []

    def copy_of(src, dst, send_sem, recv_sem, device):
        return pltpu.make_async_remote_copy(
            src_ref=src, dst_ref=dst, send_sem=send_sem, recv_sem=recv_sem,
            device_id=device, device_id_type=MESH,
        )

    def send(src, dst, send_sem, recv_sem, device):
        copy = copy_of(src, dst, send_sem, recv_sem, device)
        copy.start()
        sent.append(copy)

    def receive(dst, send_sem, recv_sem, device):
        copy_of(dst, dst, send_sem, recv_sem, device).wait_recv()

    def col(dy):
        return lax.rem(y + dy + NY, NY)

    def layer_of(dz):
        return lax.rem(z + dz + NZ, NZ)

    for dy in (1, 3, 2):
        send(tok_s.at[col(dy)], tok_y.at[y], a1s.at[dy], a1r.at[dy], ffn(0, dy))
    for dy in (1, 3, 2):
        send(aux_s.at[col(dy)], aux_y.at[y], b1s.at[dy], b1r.at[dy], ffn(0, dy))
    for dy in (1, 3, 2):
        receive(tok_y.at[col(-dy)], a1s.at[dy], a1r.at[dy], ffn(0, dy))
    for dz in (4, 3, 5, 2, 6, 1, 7):
        send(tok_y.at[:, layer_of(dz)], tok_z.at[z], a2s.at[dz], a2r.at[dz], ffn(dz, 0))
    for i in range(NY):
        tok_z[z, i] = tok_y[i, z]
    for dy in (1, 3, 2):
        receive(aux_y.at[col(-dy)], b1s.at[dy], b1r.at[dy], ffn(0, dy))
    for dz in (1, 7, 2, 6, 3, 5, 4):
        receive(tok_z.at[layer_of(-dz)], a2s.at[dz], a2r.at[dz], ffn(dz, 0))
    own_tokens = jnp.concatenate(
        [tok_z[i // NY, i % NY].astype(f32) for i in range(NZ * NY)], axis=0
    ).astype(bf16)
    tcol[...] = own_tokens
    packed = jnp.dot(pm[...].astype(bf16), own_tokens, preferred_element_type=f32).astype(bf16)
    for i in range(E):
        pks[i] = packed[i * CAP:(i + 1) * CAP, :]

    def slot_rows(c):
        return pl.ds(pl.multiple_of(c * CAP, 16), CAP)

    for d in (4, 3, 5, 2, 6, 1, 7):
        send(pks.at[lax.rem(e + d, E)], buf.at[f, slot_rows(e)], xs.at[d], xr.at[d], peer(d))
    buf[f, slot_rows(e), :] = pks[e]
    for dz in range(1, NZ):
        send(aux_y.at[:, layer_of(dz)], aux_z.at[z], b2s.at[dz], b2r.at[dz], ffn(dz, 0))
    for i in range(NY):
        aux_z[z, i] = aux_y[i, z]
    for load in late_loads:
        load.start()
    for d in (1, 7, 2, 6, 3, 5, 4):
        receive(buf.at[f, slot_rows(lax.rem(e + E - d, E))], xs.at[d], xr.at[d], peer(d))

    def gather(plan, ref, send_sems, recv_sems, after):
        done = set()
        started = set()

        def start_ready():
            for key in plan.order:
                if key not in started and all(n in done for n in plan.deps[key]):
                    started.add(key)
                    step, block, (r0, n) = plan.msgs[key]
                    view = ref.at[at(*block), pl.ds(r0, n)]
                    i = plan.index[key]
                    send(view, view, send_sems.at[i], recv_sems.at[i], ffn(*step))

        start_ready()
        for g in range(1, plan.last + 1):
            for key in plan.order:
                if plan.gen[key] == g:
                    step, block, (r0, n) = plan.msgs[key]
                    view = ref.at[at(block[0] - step[0], block[1] - step[1]), pl.ds(r0, n)]
                    i = plan.index[key]
                    receive(view, send_sems.at[i], recv_sems.at[i], ffn(*step))
                    done.add(key)
                    start_ready()
            after(g)

    def aux_part():
        for dz in range(1, NZ):
            receive(aux_z.at[layer_of(-dz)], b2s.at[dz], b2r.at[dz], ffn(dz, 0))
        logit_rows = jnp.concatenate(
            [aux_z[i // NY, i % NY, 0:4, :] for i in range(NZ * NY)], axis=0
        )
        logits = jnp.transpose(logit_rows)[0:E, :]
        total = aux_z[0, 0, 4:8, :]
        for i in range(1, NZ * NY):
            total = total + aux_z[i // NY, i % NY, 4:8, :]
        gall[y, z] = total
        for dz in range(1, NZ):
            send(gall.at[y, z], gall.at[y, z], g1s.at[dz], g1r.at[dz], ffn(dz, 0))
        picked_first = jnp.sum(jnp.where(expert_ids == first, logits, 0.0), axis=0, keepdims=True)
        picked_second = jnp.sum(
            jnp.where(expert_ids == second, logits, 0.0), axis=0, keepdims=True
        )
        weight_first = 1.0 / (1.0 + jnp.exp(picked_second - picked_first))
        weights = jnp.where(expert_ids == first, weight_first, 1.0 - weight_first)
        weighted = jnp.concatenate(
            [pm[i * CAP:(i + 1) * CAP, :] * weights[i:i + 1, :] for i in range(E)], axis=0
        )
        turned = jnp.concatenate(
            [jnp.transpose(weighted[i * 128:(i + 1) * 128, :]) for i in range(E * CAP // 128)],
            axis=1,
        )
        high = turned.astype(bf16)
        whi[...] = high
        wlo[...] = (turned - high.astype(f32)).astype(bf16)

    def gram_part():
        for dz in range(1, NZ):
            receive(gall.at[y, layer_of(-dz)], g1s.at[dz], g1r.at[dz], ffn(dz, 0))
        for dy in range(1, NY):
            send(gall.at[y], gall.at[y], g2s.at[dy], g2r.at[dy], ffn(0, dy))

    groups = {2: (0,), 3: (-1, 1), 4: (-2, 2), 5: (-3, 3), 6: (4,)}

    def expand(g):
        if g == 1:
            aux_part()
            return
        if g == 2:
            for load in loads:
                load.wait()
        if g == 3:
            gram_part()
        for dz in groups[g]:
            zz = layer_of(dz)
            lhs = jnp.concatenate([buf[zz * NY + i] for i in range(NY)], axis=1)
            for m in range(2):
                part = jnp.dot(lhs, w[m, zz], preferred_element_type=f32)
                acc[m] = part if g == 2 else acc[m] + part

    gather(SLOTS, buf, ags, agr, expand)

    gate, up = acc[0], acc[1]
    hid[...] = (gate / (1.0 + jnp.exp(-gate)) * up).astype(bf16)

    for load in late_loads:
        load.wait()
    plan = SLOTS
    got, started, made = set(), set(), set()

    def down(dz):
        zz = layer_of(dz)
        value = jnp.dot(hid[...], wd[zz], preferred_element_type=f32).astype(bf16)
        for i in range(NY):
            vb[zz * NY + i] = value[:, i * 128:(i + 1) * 128]
        made.add(dz % NZ)

    def reduce_ready():
        for key in reversed(plan.order):
            step, block, (r0, n) = plan.msgs[key]
            dest = (block[0] - step[0], block[1] - step[1])
            if (
                key not in started and dest[0] % NZ in made
                and all(u in got for u in plan.users[key])
            ):
                started.add(key)
                i = plan.index[key]
                send(
                    vb.at[at(*dest), pl.ds(r0, n)], rb.at[pl.ds(plan.offset[key], n)],
                    rss.at[i], rsr.at[i], ffn(-step[0], -step[1]),
                )

    for dz in (4, 3, -3, 2, -2, 1, -1, 0):
        down(dz)
        reduce_ready()
    for key in reversed(plan.order):
        step, block, (r0, n) = plan.msgs[key]
        i = plan.index[key]
        rows = pl.ds(plan.offset[key], n)
        receive(rb.at[rows], rss.at[i], rsr.at[i], ffn(-step[0], -step[1]))
        here = at(*block)
        vb[here, r0:r0 + n, :] = (
            vb[here, r0:r0 + n, :].astype(f32) + rb[rows, :].astype(f32)
        ).astype(bf16)
        got.add(key)
        reduce_ready()

    for d in (4, 3, 5, 2, 6, 1, 7):
        send(
            vb.at[f, slot_rows(lax.rem(e + d, E))], rx.at[slot_rows(e)],
            ys.at[d], yr.at[d], peer(d),
        )
    rx[slot_rows(e), :] = vb[f, slot_rows(e), :]
    for dy in range(1, NY):
        receive(gall.at[col(-dy)], g2s.at[dy], g2r.at[dy], ffn(0, dy))
    for d in (1, 7, 2, 6, 3, 5, 4):
        receive(rx.at[slot_rows(lax.rem(e + E - d, E))], ys.at[d], yr.at[d], peer(d))
    mixture = jnp.dot(whi[...], rx[...], preferred_element_type=f32) + jnp.dot(
        wlo[...], rx[...], preferred_element_type=f32
    )
    layer_cols = (tcol[...].astype(f32) + mixture).astype(bf16)
    lbuf[f] = layer_cols

    def contract(g):
        for dz in groups.get(g, ()):
            zz = layer_of(dz)
            block = jnp.concatenate([lbuf[zz * NY + i] for i in range(NY)], axis=1)
            gram_g = lax.dot_general(
                block, block, (((1,), (1,)), ((), ())), preferred_element_type=f32
            )
            adp_g = jnp.dot(block, ad[zz], preferred_element_type=f32)
            gram[...] = gram_g if g == 2 else gram[...] + gram_g
            adp[...] = adp_g if g == 2 else adp[...] + adp_g
            grad[zz] = lax.dot_general(
                block, up_ref[...], (((0,), (0,)), ((), ())), preferred_element_type=f32
            )

    gather(LAYER, lbuf, lgs, lgr, contract)

    whole_gram = jnp.concatenate(
        [gall[i % NY, i // NY] for i in range(NZ * NY)], axis=0
    )
    squared = jnp.sum(
        jnp.sum(gram[...] * whole_gram, axis=1, keepdims=True), axis=0, keepdims=True
    )
    limit = bound_ref[0]
    norm = jnp.sqrt(jnp.maximum(squared, 0.0))
    factor = limit / jnp.maximum(norm, limit)
    adapted_ref[...] = (layer_cols.astype(f32) + adp[...]).astype(bf16)
    for g in range(NZ):
        clipped_ref[g * 512:(g + 1) * 512, :] = (grad[g] * factor).astype(bf16)
    for copy in sent:
        copy.wait_send()


def per_device(tokens, routes, router, w_gate, w_up, w_down, adapter, upstream, bound):
    F, E = NZ * NY, 8
    R = E * CAP
    dma = pltpu.SemaphoreType.DMA
    vmem = pl.BlockSpec(memory_space=pltpu.VMEM)
    hbm = pl.BlockSpec(memory_space=pl.ANY)
    V = pltpu.VMEM
    n1, n2 = len(SLOTS.keys), len(LAYER.keys)
    scratch = [
        V((2, NZ, 512, 384), bf16), V((NZ, 384, 512), bf16), V((NZ, 512, 128), bf16),
        V((NY, NZ, 4, 128), bf16), V((NY, NZ, 4, 128), bf16), V((NZ, NY, 4, 128), bf16),
        V((NY, NZ, 8, 128), f32), V((NY, NZ, 8, 128), f32), V((NZ, NY, 8, 128), f32),
        V((NY, NZ, 4, 128), f32), V((8, 128), f32),
        V((128, 128), bf16), V((R, 128), f32), V((128, R), bf16), V((128, R), bf16),
        V((E, CAP, 128), bf16), V((F, R, 128), bf16), V((2, R, 384), f32), V((R, 384), bf16),
        V((F, R, 128), bf16), V((SLOTS.total, 128), bf16), V((R, 128), bf16),
        V((F, 128, 128), bf16), V((NZ, 512, 128), f32), V((128, 128), f32), V((128, 128), f32),
        dma((4, NZ)),
        dma((NY,)), dma((NY,)), dma((NZ,)), dma((NZ,)),
        dma((NY,)), dma((NY,)), dma((NZ,)), dma((NZ,)),
        dma((NZ,)), dma((NZ,)), dma((NY,)), dma((NY,)),
        dma((E,)), dma((E,)), dma((E,)), dma((E,)),
        dma((n1,)), dma((n1,)), dma((n1,)), dma((n1,)), dma((n2,)), dma((n2,)),
    ]
    adapted, clipped = pl.pallas_call(
        layer_kernel,
        out_shape=(
            jax.ShapeDtypeStruct((128, 128), bf16),
            jax.ShapeDtypeStruct((F * 128, 128), bf16),
        ),
        in_specs=[
            vmem, vmem, vmem, hbm, hbm, hbm, hbm, vmem,
            pl.BlockSpec(memory_space=pltpu.SMEM),
        ],
        out_specs=(vmem, vmem),
        scratch_shapes=scratch,
        compiler_params=pltpu.CompilerParams(
            collective_id=0, has_side_effects=True, vmem_limit_bytes=60_000_000
        ),
    )(
        tokens[0], routes[0].T, router.T, w_gate[0], w_up[0], w_down[0], adapter[0],
        upstream[0], bound,
    )
    return (adapted[None], clipped[None])


def solution(mesh):
    in_specs = (
        P("expert", "ffn", None),
        P("expert", None, None),
        P(),
        P("expert", None, "ffn"),
        P("expert", None, "ffn"),
        P("expert", "ffn", None),
        P("expert", None, "ffn"),
        P("expert", None, "ffn"),
        P("expert"),
    )
    out_specs = (P("expert", None, "ffn"), P("expert", None, "ffn"))
    return jax.shard_map(
        per_device, mesh=mesh, in_specs=in_specs, out_specs=out_specs, check_vma=False
    )
```

```python
import functools

import jax
import jax.numpy as jnp
from jax import lax
from jax.experimental import pallas as pl
from jax.experimental.pallas import tpu as pltpu
from jax.sharding import PartitionSpec as P

MESH = pl.DeviceIdType.MESH
NZ, NY = 8, 4
CAP = 48
bf16, f32 = jnp.bfloat16, jnp.float32


LATENCY, ROUTED, RATE = 2.45, 0.75, 46.6e3
RING, SKIP = {1: 0, 2: 1, 3: 2, 4: 3}, {1: 0, 2: 0, 3: 2, 4: 2}
YRING, YDIRECT = {1: 0, 2: 1}, {1: 0, 2: 0}


class Plan:
    def __init__(self, rows, rows_a, za, ya, yb, zb):
        half_a = -(-rows_a // 32) * 16
        rows_b = rows - rows_a
        half_b = -(-rows_b // 32) * 16
        A = ((0, rows_a), (0, half_a), (half_a, rows_a - half_a))
        B = ((rows_a, rows_b), (rows_a, half_b), (rows_a + half_b, rows_b - half_b))
        self.msgs, self.deps = {}, {}

        def line(name, parents, part, move, needs):
            last = max(parents)
            for k in sorted(parents):
                for s in (1, -1):
                    j = parents[k]
                    rows_k = part[0] if k < last else part[1 if s > 0 else 2]
                    step, block = move(s, k, j)
                    self.msgs[name + (s, k)] = (step, block, rows_k)
                    self.deps[name + (s, k)] = [name + (s, j)] if j else needs

        line(("Az",), za, A, lambda s, k, j: ((s * (k - j), 0), (-s * j, 0)), [])
        line(("By",), yb, B, lambda s, k, j: ((0, s * (k - j)), (0, -s * j)), [])
        for bz in (0, -1, 1, -2, 2, -3, 3, -4):
            needs = [] if bz == 0 else [("Az", -1 if bz > 0 else 1, abs(bz))]
            if abs(bz) == NZ // 2:
                needs = [("Az", 1, NZ // 2), ("Az", -1, NZ // 2)]
            line(("Ay", bz), ya, A, lambda s, k, j: ((0, s * (k - j)), (bz, -s * j)), needs)
        for by in (0, -1, 1, 2):
            needs = [] if by == 0 else [("By", -1 if by > 0 else 1, abs(by))]
            if abs(by) == NY // 2:
                needs = [("By", 1, NY // 2), ("By", -1, NY // 2)]
            line(("Bz", by), zb, B, lambda s, k, j: ((s * (k - j), 0), (-s * j, by)), needs)
        self.keys = list(self.msgs)
        self.index = {key: i for i, key in enumerate(self.keys)}
        self.users = {key: [u for u in self.keys if key in self.deps[u]] for key in self.keys}
        self.offset, self.total = {}, 0
        for key in self.keys:
            self.offset[key] = self.total
            self.total += self.msgs[key][2][1]

    def target(self, key):
        step, block, _ = self.msgs[key]
        return (block[0] - step[0], block[1] - step[1])

    def near(self, dz):
        return (dz + NZ // 2 - 1) % NZ - (NZ // 2 - 1)


def schedule(plan, reduce, costs, extras=()):
    cost_dot, cost_act, cost_down, cost_add = costs
    far_first = (4, 3, -3, 2, -2, 1, -1, 0)

    def shape(key):
        step, _, (_, n) = plan.msgs[key]
        return (step[0] != 0, step[0] + step[1] > 0), abs(step[0] + step[1]), n * 256 / RATE

    def tails(after):
        found = {}

        def tail(key):
            if key not in found:
                _, hops, wire = shape(key)
                found[key] = LATENCY + hops * wire + max([tail(u) for u in after[key]], default=0.0)
            return found[key]

        for key in plan.keys:
            tail(key)
        return found

    tail_of = {"gather": tails(plan.users), "reduce": tails(plan.deps)}
    waits = {"gather": plan.deps, "reduce": plan.users}
    done = {"gather": set(), "reduce": set()}
    started = {"gather": set(), "reduce": set()}
    groups = {dz: {k for k in plan.keys if plan.near(plan.target(k)[0]) == dz} for dz in far_first}
    dots, acted, downs = [], [False], []
    clock, links, flying, steps, extras = [0.0], {}, [], [], list(extras)

    def start_ready():
        ready = [("gather", k) for k in plan.keys if k not in started["gather"]
                 and all(n in done["gather"] for n in plan.deps[k])]
        if reduce:
            ready += [("reduce", k) for k in plan.keys if k not in started["reduce"]
                      and plan.near(plan.target(k)[0]) in downs
                      and all(n in done["reduce"] for n in plan.users[k])]
        ready.sort(key=lambda mk: (-tail_of[mk[0]][mk[1]], plan.index[mk[1]]))
        for mode, key in ready:
            started[mode].add(key)
            link, hops, wire = shape(key)
            if mode == "reduce":
                link = (link[0], not link[1])
            clock[0] += 0.02
            links[link] = max(clock[0], links.get(link, 0.0)) + hops * wire
            flying.append((links[link] + LATENCY + (hops - 1) * ROUTED, len(steps), mode, key))
            steps.append(("send", mode, key))

    start_ready()
    while True:
        flying.sort()
        if flying and flying[0][0] <= clock[0]:
            _, _, mode, key = flying.pop(0)
            clock[0] += 0.02 + (cost_add * plan.msgs[key][2][1] / 112 if mode == "reduce" else 0.0)
            steps.append(("recv", mode, key))
            done[mode].add(key)
            start_ready()
            continue
        full = [dz for dz in reversed(far_first) if dz not in dots and groups[dz] <= done["gather"]]
        if extras and extras[0][1] <= clock[0]:
            name, _, cost = extras.pop(0)
            steps.append(("extra", name, None))
            clock[0] += cost
        elif full:
            dots.append(full[0])
            steps.append(("dot", full[0], len(dots) == 1))
            clock[0] += cost_dot
        elif reduce and len(dots) == NZ and not acted[0]:
            acted[0] = True
            steps.append(("act", None, None))
            clock[0] += cost_act
        elif acted[0] and len(downs) < NZ:
            downs.append(far_first[len(downs)])
            steps.append(("down", downs[-1], None))
            clock[0] += cost_down
            start_ready()
        elif flying:
            clock[0] = max(clock[0], flying[0][0])
        else:
            return steps


SLOTS = Plan(8 * CAP, 224, SKIP, YRING, YDIRECT, RING)
LAYER = Plan(128, 80, SKIP, YDIRECT, YRING, SKIP)
SLOT_STEPS = schedule(
    SLOTS, True, (0.45, 0.2, 0.25, 0.06), (("aux", 1.0, 1.0), ("gram", 7.0, 0.1))
)
LAYER_STEPS = schedule(LAYER, False, (0.15, 0.0, 0.0, 0.0))


def layer_kernel(
    tok_hbm, routes_hbm, router_hbm, wg_hbm, wu_hbm, wd_hbm, ad_hbm, up_hbm, bound_ref,
    layer_hbm, adapted_ref, factor_ref,
    tok_ref, routes_ref, router_ref, up_ref, w, wd, ad, tok_s, tok_y, tok_z, aux_s, aux_y, aux_z, gall, lgp, tcol, pm, whi, wlo,
    pks, buf, acc, hid, vb, rb, rx, lbuf, gram, adp,
    in_sem, out_sem, w_sem, a1s, a1r, a2s, a2r, b1s, b1r, b2s, b2r, g1s, g1r, g2s, g2r,
    xs, xr, ys, yr, ags, agr, rss, rsr, lgs, lgr,
):
    E = 8
    D = NZ * NY * 128
    e = lax.axis_index("expert")
    f = lax.axis_index("ffn")
    z, y = f // NY, lax.rem(f, NY)

    loads = []
    for g in range(NZ):
        rows = pl.ds(g * 512, 512)
        loads.append(pltpu.make_async_copy(wg_hbm.at[rows, :], w.at[0, g], w_sem.at[0, g]))
        loads.append(pltpu.make_async_copy(wu_hbm.at[rows, :], w.at[1, g], w_sem.at[1, g]))
    late_loads = []
    for g in range(NZ):
        late_loads.append(pltpu.make_async_copy(
            wd_hbm.at[:, pl.ds(g * 512, 512)], wd.at[g], w_sem.at[2, g]))
        late_loads.append(pltpu.make_async_copy(
            ad_hbm.at[pl.ds(g * 512, 512), :], ad.at[g], w_sem.at[3, g]))

    def at(dz, dy):
        return lax.rem(z + dz + NZ, NZ) * NY + lax.rem(y + dy + NY, NY)

    def ffn(dz, dy):
        return {"ffn": at(dz, dy)}

    def peer(d):
        return {"expert": lax.rem(e + d, E)}

    barrier = pltpu.get_barrier_semaphore()
    for dy in range(1, NY):
        pl.semaphore_signal(barrier, inc=1, device_id=ffn(0, dy), device_id_type=MESH)
    for dz in range(1, NZ):
        pl.semaphore_signal(barrier, inc=1, device_id=ffn(dz, 0), device_id_type=MESH)
    for d in range(1, E):
        pl.semaphore_signal(barrier, inc=1, device_id=peer(d), device_id_type=MESH)

    small = [
        pltpu.make_async_copy(src, dst, in_sem.at[i])
        for i, (src, dst) in enumerate((
            (tok_hbm, tok_ref), (up_hbm, up_ref), (router_hbm, router_ref),
            (routes_hbm, routes_ref),
        ))
    ]
    for load in small + loads:
        load.start()
    for load in small:
        load.wait()

    for i in range(NZ * NY):
        tok_s[i % NY, i // NY] = tok_ref[:, i * 128:(i + 1) * 128]
    tok_y[y] = tok_s[y]
    lgp[...] = jnp.zeros_like(lgp)
    lgp[0:4, 0:E] = lax.dot_general(
        tok_ref[...], router_ref[...], (((1,), (1,)), ((), ())), preferred_element_type=f32
    )
    own_logits = lgp[0:4, :]
    own_gram = lax.dot_general(
        up_ref[...], up_ref[...], (((1,), (1,)), ((), ())), preferred_element_type=f32
    )
    for i in range(NZ * NY):
        aux_s[i % NY, i // NY, 0:4, :] = own_logits
        aux_s[i % NY, i // NY, 4:8, :] = own_gram[4 * i:4 * i + 4, :]
    aux_y[y] = aux_s[y]

    first, second = routes_ref[0:1, :], routes_ref[1:2, :]
    expert_ids = lax.broadcasted_iota(jnp.int32, (E, 128), 0)
    hits = ((expert_ids == first) | (expert_ids == second)).astype(f32)
    before = (
        lax.broadcasted_iota(jnp.int32, (128, 128), 0)
        < lax.broadcasted_iota(jnp.int32, (128, 128), 1)
    ).astype(f32)
    rank = jnp.dot(hits.astype(bf16), before.astype(bf16), preferred_element_type=f32)
    slot = jnp.where(hits > 0.0, rank, -1.0)
    slot_ids = lax.broadcasted_iota(jnp.int32, (CAP, 128), 0).astype(f32)
    for i in range(E):
        pm[i * CAP:(i + 1) * CAP, :] = (slot_ids == slot[i:i + 1, :]).astype(f32)

    pl.semaphore_wait(barrier, NY - 1 + NZ - 1 + E - 1)

    sent = []

    def copy_of(src, dst, send_sem, recv_sem, device):
        return pltpu.make_async_remote_copy(
            src_ref=src, dst_ref=dst, send_sem=send_sem, recv_sem=recv_sem,
            device_id=device, device_id_type=MESH,
        )

    def send(src, dst, send_sem, recv_sem, device):
        copy = copy_of(src, dst, send_sem, recv_sem, device)
        copy.start()
        sent.append(copy)

    def receive(dst, send_sem, recv_sem, device):
        copy_of(dst, dst, send_sem, recv_sem, device).wait_recv()

    def col(dy):
        return lax.rem(y + dy + NY, NY)

    def layer_of(dz):
        return lax.rem(z + dz + NZ, NZ)

    for dy in (1, 3, 2):
        send(tok_s.at[col(dy)], tok_y.at[y], a1s.at[dy], a1r.at[dy], ffn(0, dy))
    for dy in (1, 3, 2):
        send(aux_s.at[col(dy)], aux_y.at[y], b1s.at[dy], b1r.at[dy], ffn(0, dy))
    for dy in (1, 3, 2):
        receive(tok_y.at[col(-dy)], a1s.at[dy], a1r.at[dy], ffn(0, dy))
    for dz in (4, 3, 5, 2, 6, 1, 7):
        send(tok_y.at[:, layer_of(dz)], tok_z.at[z], a2s.at[dz], a2r.at[dz], ffn(dz, 0))
    for i in range(NY):
        tok_z[z, i] = tok_y[i, z]
    for dy in (1, 3, 2):
        receive(aux_y.at[col(-dy)], b1s.at[dy], b1r.at[dy], ffn(0, dy))
    for dz in (1, 7, 2, 6, 3, 5, 4):
        receive(tok_z.at[layer_of(-dz)], a2s.at[dz], a2r.at[dz], ffn(dz, 0))
    own_tokens = jnp.concatenate(
        [tok_z[i // NY, i % NY].astype(f32) for i in range(NZ * NY)], axis=0
    ).astype(bf16)
    tcol[...] = own_tokens
    packed = jnp.dot(pm[...].astype(bf16), own_tokens, preferred_element_type=f32).astype(bf16)
    for i in range(E):
        pks[i] = packed[i * CAP:(i + 1) * CAP, :]

    def slot_rows(c):
        return pl.ds(pl.multiple_of(c * CAP, 16), CAP)

    for d in (4, 3, 5, 2, 6, 1, 7):
        send(pks.at[lax.rem(e + d, E)], buf.at[f, slot_rows(e)], xs.at[d], xr.at[d], peer(d))
    buf[f, slot_rows(e), :] = pks[e]
    for dz in range(1, NZ):
        send(aux_y.at[:, layer_of(dz)], aux_z.at[z], b2s.at[dz], b2r.at[dz], ffn(dz, 0))
    for i in range(NY):
        aux_z[z, i] = aux_y[i, z]
    for load in late_loads:
        load.start()
    for d in (1, 7, 2, 6, 3, 5, 4):
        receive(buf.at[f, slot_rows(lax.rem(e + E - d, E))], xs.at[d], xr.at[d], peer(d))

    def aux_part():
        for dz in range(1, NZ):
            receive(aux_z.at[layer_of(-dz)], b2s.at[dz], b2r.at[dz], ffn(dz, 0))
        logit_rows = jnp.concatenate(
            [aux_z[i // NY, i % NY, 0:4, :] for i in range(NZ * NY)], axis=0
        )
        logits = jnp.transpose(logit_rows)[0:E, :]
        total = aux_z[0, 0, 4:8, :]
        for i in range(1, NZ * NY):
            total = total + aux_z[i // NY, i % NY, 4:8, :]
        gall[y, z] = total
        for dz in range(1, NZ):
            send(gall.at[y, z], gall.at[y, z], g1s.at[dz], g1r.at[dz], ffn(dz, 0))
        picked_first = jnp.sum(jnp.where(expert_ids == first, logits, 0.0), axis=0, keepdims=True)
        picked_second = jnp.sum(
            jnp.where(expert_ids == second, logits, 0.0), axis=0, keepdims=True
        )
        weight_first = 1.0 / (1.0 + jnp.exp(picked_second - picked_first))
        weights = jnp.where(expert_ids == first, weight_first, 1.0 - weight_first)
        weighted = jnp.concatenate(
            [pm[i * CAP:(i + 1) * CAP, :] * weights[i:i + 1, :] for i in range(E)], axis=0
        )
        turned = jnp.concatenate(
            [jnp.transpose(weighted[i * 128:(i + 1) * 128, :]) for i in range(E * CAP // 128)],
            axis=1,
        )
        high = turned.astype(bf16)
        whi[...] = high
        wlo[...] = (turned - high.astype(f32)).astype(bf16)

    def gram_part():
        for dz in range(1, NZ):
            receive(gall.at[y, layer_of(-dz)], g1s.at[dz], g1r.at[dz], ffn(dz, 0))
        for dy in range(1, NY):
            send(gall.at[y], gall.at[y], g2s.at[dy], g2r.at[dy], ffn(0, dy))

    def gather_send(plan, ref, sems, key):
        step, block, (r0, n) = plan.msgs[key]
        view = ref.at[at(*block), pl.ds(r0, n)]
        i = plan.index[key]
        send(view, view, sems[0].at[i], sems[1].at[i], ffn(*step))

    def gather_receive(plan, ref, sems, key):
        step, _, (r0, n) = plan.msgs[key]
        view = ref.at[at(*plan.target(key)), pl.ds(r0, n)]
        i = plan.index[key]
        receive(view, sems[0].at[i], sems[1].at[i], ffn(*step))

    def reduce_send(plan, key):
        step, _, (r0, n) = plan.msgs[key]
        i = plan.index[key]
        send(
            vb.at[at(*plan.target(key)), pl.ds(r0, n)], rb.at[pl.ds(plan.offset[key], n)],
            rss.at[i], rsr.at[i], ffn(-step[0], -step[1]),
        )

    def reduce_receive(plan, key):
        step, block, (r0, n) = plan.msgs[key]
        i = plan.index[key]
        rows = pl.ds(plan.offset[key], n)
        receive(rb.at[rows], rss.at[i], rsr.at[i], ffn(-step[0], -step[1]))
        here = at(*block)
        vb[here, r0:r0 + n, :] = (
            vb[here, r0:r0 + n, :].astype(f32) + rb[rows, :].astype(f32)
        ).astype(bf16)

    def expand(dz, opening):
        if opening:
            for load in loads:
                load.wait()
        zz = layer_of(dz)
        lhs = jnp.concatenate([buf[zz * NY + i] for i in range(NY)], axis=1)
        for m in range(2):
            part = jnp.dot(lhs, w[m, zz], preferred_element_type=f32)
            acc[m] = part if opening else acc[m] + part

    def activate():
        gate, up = acc[0], acc[1]
        hid[...] = (gate / (1.0 + jnp.exp(-gate)) * up).astype(bf16)
        for load in late_loads:
            load.wait()

    def down(dz):
        zz = layer_of(dz)
        value = jnp.dot(hid[...], wd[zz], preferred_element_type=f32).astype(bf16)
        for i in range(NY):
            vb[zz * NY + i] = value[:, i * 128:(i + 1) * 128]

    for kind, first_arg, second_arg in SLOT_STEPS:
        if kind == "send" and first_arg == "gather":
            gather_send(SLOTS, buf, (ags, agr), second_arg)
        elif kind == "recv" and first_arg == "gather":
            gather_receive(SLOTS, buf, (ags, agr), second_arg)
        elif kind == "send":
            reduce_send(SLOTS, second_arg)
        elif kind == "recv":
            reduce_receive(SLOTS, second_arg)
        elif kind == "dot":
            expand(first_arg, second_arg)
        elif kind == "act":
            activate()
        elif kind == "down":
            down(first_arg)
        elif first_arg == "aux":
            aux_part()
        else:
            gram_part()

    for d in (4, 3, 5, 2, 6, 1, 7):
        send(
            vb.at[f, slot_rows(lax.rem(e + d, E))], rx.at[slot_rows(e)],
            ys.at[d], yr.at[d], peer(d),
        )
    rx[slot_rows(e), :] = vb[f, slot_rows(e), :]
    for dy in range(1, NY):
        receive(gall.at[col(-dy)], g2s.at[dy], g2r.at[dy], ffn(0, dy))
    for d in (1, 7, 2, 6, 3, 5, 4):
        receive(rx.at[slot_rows(lax.rem(e + E - d, E))], ys.at[d], yr.at[d], peer(d))
    mixture = jnp.dot(whi[...], rx[...], preferred_element_type=f32) + jnp.dot(
        wlo[...], rx[...], preferred_element_type=f32
    )
    layer_cols = tcol[...].astype(f32) + mixture
    lbuf[f] = jnp.transpose(layer_cols).astype(bf16)
    outs = []

    def contract(dz, opening):
        zz = layer_of(dz)
        blocks = pl.ds(zz * NY, NY)
        out = pltpu.make_async_copy(lbuf.at[blocks], layer_hbm.at[blocks], out_sem.at[len(outs)])
        out.start()
        outs.append(out)
        block = jnp.concatenate([lbuf[zz * NY + i] for i in range(NY)], axis=0)
        turned = (((0,), (0,)), ((), ()))
        gram_g = lax.dot_general(block, block, turned, preferred_element_type=f32)
        adp_g = lax.dot_general(block, ad[zz], turned, preferred_element_type=f32)
        gram[...] = gram_g if opening else gram[...] + gram_g
        adp[...] = adp_g if opening else adp[...] + adp_g

    for kind, first_arg, second_arg in LAYER_STEPS:
        if kind == "send":
            gather_send(LAYER, lbuf, (lgs, lgr), second_arg)
        elif kind == "recv":
            gather_receive(LAYER, lbuf, (lgs, lgr), second_arg)
        else:
            contract(first_arg, second_arg)

    whole_gram = jnp.concatenate(
        [gall[i % NY, i // NY] for i in range(NZ * NY)], axis=0
    )
    squared = jnp.sum(
        jnp.sum(gram[...] * whole_gram, axis=1, keepdims=True), axis=0, keepdims=True
    )
    limit = bound_ref[0]
    norm = jnp.sqrt(jnp.maximum(squared, 0.0))
    factor_ref[...] = jnp.broadcast_to(limit / jnp.maximum(norm, limit), factor_ref.shape)
    own_cols = layer_cols.astype(bf16).astype(f32)
    adapted_ref[...] = (own_cols + adp[...]).astype(bf16)
    for copy in sent:
        copy.wait_send()
    for out in outs:
        out.wait()


def grad_kernel(
    layer_hbm, up_hbm, factor_hbm, adapted_hbm, adapted_out, clipped_hbm,
    layer, up, factor, adapted, blocks, in_sem, small_sem, out_sem,
):
    small = [
        pltpu.make_async_copy(src, dst, small_sem.at[i])
        for i, (src, dst) in enumerate((
            (up_hbm, up), (factor_hbm, factor), (adapted_hbm, adapted),
        ))
    ]
    loads = [
        pltpu.make_async_copy(layer_hbm.at[pl.ds(g * NY, NY)], layer.at[g], in_sem.at[g])
        for g in range(NZ)
    ]
    for load in small + loads:
        load.start()
    for load in small:
        load.wait()
    last = pltpu.make_async_copy(adapted, adapted_out, small_sem.at[3])
    last.start()
    stores = []
    scale = factor[0:1, 0:1]
    for g in range(NZ):
        loads[g].wait()
        part = jnp.concatenate([layer[g, i] for i in range(NY)], axis=0)
        grad = jnp.dot(part, up[...], preferred_element_type=f32)
        blocks[g] = (grad * scale).astype(bf16)
        store = pltpu.make_async_copy(
            blocks.at[g], clipped_hbm.at[pl.ds(g * 512, 512), :], out_sem.at[g]
        )
        store.start()
        stores.append(store)
    last.wait()
    for store in stores:
        store.wait()


def per_device(tokens, routes, router, w_gate, w_up, w_down, adapter, upstream, bound):
    F, E = NZ * NY, 8
    R = E * CAP
    dma = pltpu.SemaphoreType.DMA
    vmem = pl.BlockSpec(memory_space=pltpu.VMEM)
    hbm = pl.BlockSpec(memory_space=pl.ANY)
    V = pltpu.VMEM
    n1, n2 = len(SLOTS.keys), len(LAYER.keys)
    scratch = [
        V((4, NZ * NY * 128), bf16), V((2, 128), jnp.int32), V((E, NZ * NY * 128), bf16),
        V((128, 128), bf16),
        V((2, NZ, 512, 384), bf16), V((NZ, 384, 512), bf16), V((NZ, 512, 128), bf16),
        V((NY, NZ, 4, 128), bf16), V((NY, NZ, 4, 128), bf16), V((NZ, NY, 4, 128), bf16),
        V((NY, NZ, 8, 128), f32), V((NY, NZ, 8, 128), f32), V((NZ, NY, 8, 128), f32),
        V((NY, NZ, 4, 128), f32), V((8, 128), f32),
        V((128, 128), bf16), V((R, 128), f32), V((128, R), bf16), V((128, R), bf16),
        V((E, CAP, 128), bf16), V((F, R, 128), bf16), V((2, R, 384), f32), V((R, 384), bf16),
        V((F, R, 128), bf16), V((SLOTS.total, 128), bf16), V((R, 128), bf16),
        V((F, 128, 128), bf16), V((128, 128), f32), V((128, 128), f32),
        dma((4,)), dma((NZ,)), dma((4, NZ)),
        dma((NY,)), dma((NY,)), dma((NZ,)), dma((NZ,)),
        dma((NY,)), dma((NY,)), dma((NZ,)), dma((NZ,)),
        dma((NZ,)), dma((NZ,)), dma((NY,)), dma((NY,)),
        dma((E,)), dma((E,)), dma((E,)), dma((E,)),
        dma((n1,)), dma((n1,)), dma((n1,)), dma((n1,)), dma((n2,)), dma((n2,)),
    ]
    layer, adapted, factor = pl.pallas_call(
        layer_kernel,
        out_shape=(
            jax.ShapeDtypeStruct((F, 128, 128), bf16),
            jax.ShapeDtypeStruct((128, 128), bf16),
            jax.ShapeDtypeStruct((8, 128), f32),
        ),
        in_specs=[hbm] * 8 + [pl.BlockSpec(memory_space=pltpu.SMEM)],
        out_specs=(hbm, vmem, vmem),
        scratch_shapes=scratch,
        compiler_params=pltpu.CompilerParams(
            collective_id=0, has_side_effects=True, vmem_limit_bytes=60_000_000
        ),
    )(
        tokens[0], routes[0].T, router.T, w_gate[0], w_up[0], w_down[0], adapter[0],
        upstream[0], bound,
    )
    adapted, clipped = pl.pallas_call(
        grad_kernel,
        out_shape=(
            jax.ShapeDtypeStruct((128, 128), bf16),
            jax.ShapeDtypeStruct((F * 128, 128), bf16),
        ),
        in_specs=[hbm] * 4,
        out_specs=(hbm, hbm),
        scratch_shapes=[
            V((NZ, NY, 128, 128), bf16), V((128, 128), bf16), V((8, 128), f32),
            V((128, 128), bf16), V((NZ, 512, 128), bf16),
            dma((NZ,)), dma((4,)), dma((NZ,)),
        ],
    )(layer, upstream[0], factor, adapted)
    return (adapted[None], clipped[None])


def solution(mesh):
    in_specs = (
        P("expert", "ffn", None),
        P("expert", None, None),
        P(),
        P("expert", None, "ffn"),
        P("expert", None, "ffn"),
        P("expert", "ffn", None),
        P("expert", None, "ffn"),
        P("expert", None, "ffn"),
        P("expert"),
    )
    out_specs = (P("expert", None, "ffn"), P("expert", None, "ffn"))
    return jax.shard_map(
        per_device, mesh=mesh, in_specs=in_specs, out_specs=out_specs, check_vma=False
    )
```

```python
import functools

import jax
import jax.numpy as jnp
from jax import lax
from jax.experimental import pallas as pl
from jax.experimental.pallas import tpu as pltpu
from jax.sharding import PartitionSpec as P

MESH = pl.DeviceIdType.MESH
NZ, NY = 8, 4
CAP = 48
bf16, f32 = jnp.bfloat16, jnp.float32


LATENCY, ROUTED, RATE = 2.45, 0.75, 46.6e3
RING, SKIP = {1: 0, 2: 1, 3: 2, 4: 3}, {1: 0, 2: 0, 3: 2, 4: 2}
YRING, YDIRECT = {1: 0, 2: 1}, {1: 0, 2: 0}


class Plan:
    def __init__(self, rows, rows_a, za, ya, yb, zb):
        half_a = -(-rows_a // 32) * 16
        rows_b = rows - rows_a
        half_b = -(-rows_b // 32) * 16
        A = ((0, rows_a), (0, half_a), (half_a, rows_a - half_a))
        B = ((rows_a, rows_b), (rows_a, half_b), (rows_a + half_b, rows_b - half_b))
        self.msgs, self.deps = {}, {}

        def line(name, parents, part, move, needs):
            last = max(parents)
            for k in sorted(parents):
                for s in (1, -1):
                    j = parents[k]
                    rows_k = part[0] if k < last else part[1 if s > 0 else 2]
                    step, block = move(s, k, j)
                    self.msgs[name + (s, k)] = (step, block, rows_k)
                    self.deps[name + (s, k)] = [name + (s, j)] if j else needs

        line(("Az",), za, A, lambda s, k, j: ((s * (k - j), 0), (-s * j, 0)), [])
        line(("By",), yb, B, lambda s, k, j: ((0, s * (k - j)), (0, -s * j)), [])
        for bz in (0, -1, 1, -2, 2, -3, 3, -4):
            needs = [] if bz == 0 else [("Az", -1 if bz > 0 else 1, abs(bz))]
            if abs(bz) == NZ // 2:
                needs = [("Az", 1, NZ // 2), ("Az", -1, NZ // 2)]
            line(("Ay", bz), ya, A, lambda s, k, j: ((0, s * (k - j)), (bz, -s * j)), needs)
        for by in (0, -1, 1, 2):
            needs = [] if by == 0 else [("By", -1 if by > 0 else 1, abs(by))]
            if abs(by) == NY // 2:
                needs = [("By", 1, NY // 2), ("By", -1, NY // 2)]
            line(("Bz", by), zb, B, lambda s, k, j: ((s * (k - j), 0), (-s * j, by)), needs)
        self.keys = list(self.msgs)
        self.index = {key: i for i, key in enumerate(self.keys)}
        self.users = {key: [u for u in self.keys if key in self.deps[u]] for key in self.keys}
        self.offset, self.total = {}, 0
        for key in self.keys:
            self.offset[key] = self.total
            self.total += self.msgs[key][2][1]

    def target(self, key):
        step, block, _ = self.msgs[key]
        return (block[0] - step[0], block[1] - step[1])

    def near(self, dz):
        return (dz + NZ // 2 - 1) % NZ - (NZ // 2 - 1)


def schedule(plan, reduce, costs, extras=()):
    cost_dot, cost_act, cost_down, cost_add = costs
    far_first = (4, 3, -3, 2, -2, 1, -1, 0)

    def shape(key):
        step, _, (_, n) = plan.msgs[key]
        return (step[0] != 0, step[0] + step[1] > 0), abs(step[0] + step[1]), n * 256 / RATE

    def tails(after):
        found = {}

        def tail(key):
            if key not in found:
                _, hops, wire = shape(key)
                found[key] = LATENCY + hops * wire + max([tail(u) for u in after[key]], default=0.0)
            return found[key]

        for key in plan.keys:
            tail(key)
        return found

    tail_of = {"gather": tails(plan.users), "reduce": tails(plan.deps)}
    waits = {"gather": plan.deps, "reduce": plan.users}
    done = {"gather": set(), "reduce": set()}
    started = {"gather": set(), "reduce": set()}
    groups = {dz: {k for k in plan.keys if plan.near(plan.target(k)[0]) == dz} for dz in far_first}
    dots, acted, downs = [], [False], []
    clock, links, flying, steps, extras = [0.0], {}, [], [], list(extras)

    def start_ready():
        ready = [("gather", k) for k in plan.keys if k not in started["gather"]
                 and all(n in done["gather"] for n in plan.deps[k])]
        if reduce:
            ready += [("reduce", k) for k in plan.keys if k not in started["reduce"]
                      and plan.near(plan.target(k)[0]) in downs
                      and all(n in done["reduce"] for n in plan.users[k])]
        ready.sort(key=lambda mk: (-tail_of[mk[0]][mk[1]], plan.index[mk[1]]))
        for mode, key in ready:
            started[mode].add(key)
            link, hops, wire = shape(key)
            if mode == "reduce":
                link = (link[0], not link[1])
            clock[0] += 0.02
            links[link] = max(clock[0], links.get(link, 0.0)) + hops * wire
            flying.append((links[link] + LATENCY + (hops - 1) * ROUTED, len(steps), mode, key))
            steps.append(("send", mode, key))

    start_ready()
    while True:
        flying.sort()
        if flying and flying[0][0] <= clock[0]:
            _, _, mode, key = flying.pop(0)
            clock[0] += 0.02 + (cost_add * plan.msgs[key][2][1] / 112 if mode == "reduce" else 0.0)
            steps.append(("recv", mode, key))
            done[mode].add(key)
            start_ready()
            continue
        full = [dz for dz in reversed(far_first) if dz not in dots and groups[dz] <= done["gather"]]
        if extras and extras[0][1] <= clock[0]:
            name, _, cost = extras.pop(0)
            steps.append(("extra", name, None))
            clock[0] += cost
        elif full:
            dots.append(full[0])
            steps.append(("dot", full[0], len(dots) == 1))
            clock[0] += cost_dot
        elif reduce and len(dots) == NZ and not acted[0]:
            acted[0] = True
            steps.append(("act", None, None))
            clock[0] += cost_act
        elif acted[0] and len(downs) < NZ:
            downs.append(far_first[len(downs)])
            steps.append(("down", downs[-1], None))
            clock[0] += cost_down
            start_ready()
        elif flying:
            clock[0] = max(clock[0], flying[0][0])
        else:
            return steps


SLOTS = Plan(8 * CAP, 224, SKIP, YRING, YDIRECT, RING)
LAYER = Plan(128, 80, SKIP, YDIRECT, YRING, SKIP)
SLOT_STEPS = schedule(
    SLOTS, True, (0.45, 0.2, 0.25, 0.06), (("aux", 1.0, 1.0), ("gram", 7.0, 0.1))
)
LAYER_STEPS = schedule(LAYER, False, (0.15, 0.0, 0.0, 0.0))


def layer_kernel(
    tok_hbm, routes_hbm, router_hbm, wg_hbm, wu_hbm, wd_hbm, ad_hbm, up_hbm, bound_ref,
    layer_hbm, adapted_ref, factor_ref,
    tok_ref, routes_ref, router_ref, up_ref, w, wd, ad, tok_s, tok_y, tok_z, aux_s, aux_y, aux_z, gall, lgp, tcol, pm, whi, wlo,
    pks, buf, acc, hid, vb, rb, rx, lbuf, gram, adp,
    in_sem, out_sem, w_sem, a1s, a1r, a2s, a2r, b1s, b1r, b2s, b2r, g1s, g1r, g2s, g2r,
    xs, xr, ys, yr, ags, agr, rss, rsr, lgs, lgr,
):
    E = 8
    D = NZ * NY * 128
    e = lax.axis_index("expert")
    f = lax.axis_index("ffn")
    z, y = f // NY, lax.rem(f, NY)

    loads = []
    for g in range(NZ):
        rows = pl.ds(g * 512, 512)
        loads.append(pltpu.make_async_copy(wg_hbm.at[rows, :], w.at[0, g], w_sem.at[0, g]))
        loads.append(pltpu.make_async_copy(wu_hbm.at[rows, :], w.at[1, g], w_sem.at[1, g]))
    late_loads = []
    for g in range(NZ):
        late_loads.append(pltpu.make_async_copy(
            wd_hbm.at[:, pl.ds(g * 512, 512)], wd.at[g], w_sem.at[2, g]))
        late_loads.append(pltpu.make_async_copy(
            ad_hbm.at[pl.ds(g * 512, 512), :], ad.at[g], w_sem.at[3, g]))

    def at(dz, dy):
        return lax.rem(z + dz + NZ, NZ) * NY + lax.rem(y + dy + NY, NY)

    def ffn(dz, dy):
        return {"ffn": at(dz, dy)}

    def peer(d):
        return {"expert": lax.rem(e + d, E)}

    barrier = pltpu.get_barrier_semaphore()
    for dy in range(1, NY):
        pl.semaphore_signal(barrier, inc=1, device_id=ffn(0, dy), device_id_type=MESH)
    for dz in range(1, NZ):
        pl.semaphore_signal(barrier, inc=1, device_id=ffn(dz, 0), device_id_type=MESH)
    for d in range(1, E):
        pl.semaphore_signal(barrier, inc=1, device_id=peer(d), device_id_type=MESH)

    small = [
        pltpu.make_async_copy(src, dst, in_sem.at[i])
        for i, (src, dst) in enumerate((
            (tok_hbm, tok_ref), (up_hbm, up_ref), (router_hbm, router_ref),
            (routes_hbm, routes_ref),
        ))
    ]
    for load in small + loads:
        load.start()
    for load in small:
        load.wait()

    for i in range(NZ * NY):
        tok_s[i % NY, i // NY] = tok_ref[:, i * 128:(i + 1) * 128]
    tok_y[y] = tok_s[y]
    lgp[...] = jnp.zeros_like(lgp)
    lgp[0:4, 0:E] = lax.dot_general(
        tok_ref[...], router_ref[...], (((1,), (1,)), ((), ())), preferred_element_type=f32
    )
    own_logits = lgp[0:4, :]
    own_gram = lax.dot_general(
        up_ref[...], up_ref[...], (((1,), (1,)), ((), ())), preferred_element_type=f32
    )
    for i in range(NZ * NY):
        aux_s[i % NY, i // NY, 0:4, :] = own_logits
        aux_s[i % NY, i // NY, 4:8, :] = own_gram[4 * i:4 * i + 4, :]
    aux_y[y] = aux_s[y]

    first, second = routes_ref[0:1, :], routes_ref[1:2, :]
    expert_ids = lax.broadcasted_iota(jnp.int32, (E, 128), 0)
    hits = ((expert_ids == first) | (expert_ids == second)).astype(f32)
    before = (
        lax.broadcasted_iota(jnp.int32, (128, 128), 0)
        < lax.broadcasted_iota(jnp.int32, (128, 128), 1)
    ).astype(f32)
    rank = jnp.dot(hits.astype(bf16), before.astype(bf16), preferred_element_type=f32)
    slot = jnp.where(hits > 0.0, rank, -1.0)
    slot_ids = lax.broadcasted_iota(jnp.int32, (CAP, 128), 0).astype(f32)
    for i in range(E):
        pm[i * CAP:(i + 1) * CAP, :] = (slot_ids == slot[i:i + 1, :]).astype(f32)

    pl.semaphore_wait(barrier, NY - 1 + NZ - 1 + E - 1)

    sent = []

    def copy_of(src, dst, send_sem, recv_sem, device):
        return pltpu.make_async_remote_copy(
            src_ref=src, dst_ref=dst, send_sem=send_sem, recv_sem=recv_sem,
            device_id=device, device_id_type=MESH,
        )

    def send(src, dst, send_sem, recv_sem, device):
        copy = copy_of(src, dst, send_sem, recv_sem, device)
        copy.start()
        sent.append(copy)

    def receive(dst, send_sem, recv_sem, device):
        copy_of(dst, dst, send_sem, recv_sem, device).wait_recv()

    def col(dy):
        return lax.rem(y + dy + NY, NY)

    def layer_of(dz):
        return lax.rem(z + dz + NZ, NZ)

    for dy in (1, 3, 2):
        send(tok_s.at[col(dy)], tok_y.at[y], a1s.at[dy], a1r.at[dy], ffn(0, dy))
    for dy in (1, 3, 2):
        send(aux_s.at[col(dy)], aux_y.at[y], b1s.at[dy], b1r.at[dy], ffn(0, dy))
    for dy in (1, 3, 2):
        receive(tok_y.at[col(-dy)], a1s.at[dy], a1r.at[dy], ffn(0, dy))
    for dz in (4, 3, 5, 2, 6, 1, 7):
        send(tok_y.at[:, layer_of(dz)], tok_z.at[z], a2s.at[dz], a2r.at[dz], ffn(dz, 0))
    for i in range(NY):
        tok_z[z, i] = tok_y[i, z]
    for dy in (1, 3, 2):
        receive(aux_y.at[col(-dy)], b1s.at[dy], b1r.at[dy], ffn(0, dy))
    for dz in (1, 7, 2, 6, 3, 5, 4):
        receive(tok_z.at[layer_of(-dz)], a2s.at[dz], a2r.at[dz], ffn(dz, 0))
    own_tokens = jnp.concatenate(
        [tok_z[i // NY, i % NY].astype(f32) for i in range(NZ * NY)], axis=0
    ).astype(bf16)
    tcol[...] = own_tokens
    packed = jnp.dot(pm[...].astype(bf16), own_tokens, preferred_element_type=f32).astype(bf16)
    for i in range(E):
        pks[i] = packed[i * CAP:(i + 1) * CAP, :]

    def slot_rows(c):
        return pl.ds(pl.multiple_of(c * CAP, 16), CAP)

    for d in (4, 3, 5, 2, 6, 1, 7):
        send(pks.at[lax.rem(e + d, E)], buf.at[f, slot_rows(e)], xs.at[d], xr.at[d], peer(d))
    buf[f, slot_rows(e), :] = pks[e]
    for dz in range(1, NZ):
        send(aux_y.at[:, layer_of(dz)], aux_z.at[z], b2s.at[dz], b2r.at[dz], ffn(dz, 0))
    for i in range(NY):
        aux_z[z, i] = aux_y[i, z]
    for load in late_loads:
        load.start()
    for d in (1, 7, 2, 6, 3, 5, 4):
        receive(buf.at[f, slot_rows(lax.rem(e + E - d, E))], xs.at[d], xr.at[d], peer(d))

    def aux_part():
        for dz in range(1, NZ):
            receive(aux_z.at[layer_of(-dz)], b2s.at[dz], b2r.at[dz], ffn(dz, 0))
        logit_rows = jnp.concatenate(
            [aux_z[i // NY, i % NY, 0:4, :] for i in range(NZ * NY)], axis=0
        )
        logits = jnp.transpose(logit_rows)[0:E, :]
        total = aux_z[0, 0, 4:8, :]
        for i in range(1, NZ * NY):
            total = total + aux_z[i // NY, i % NY, 4:8, :]
        gall[y, z] = total
        for dz in range(1, NZ):
            send(gall.at[y, z], gall.at[y, z], g1s.at[dz], g1r.at[dz], ffn(dz, 0))
        picked_first = jnp.sum(jnp.where(expert_ids == first, logits, 0.0), axis=0, keepdims=True)
        picked_second = jnp.sum(
            jnp.where(expert_ids == second, logits, 0.0), axis=0, keepdims=True
        )
        weight_first = 1.0 / (1.0 + jnp.exp(picked_second - picked_first))
        weights = jnp.where(expert_ids == first, weight_first, 1.0 - weight_first)
        weighted = jnp.concatenate(
            [pm[i * CAP:(i + 1) * CAP, :] * weights[i:i + 1, :] for i in range(E)], axis=0
        )
        turned = jnp.concatenate(
            [jnp.transpose(weighted[i * 128:(i + 1) * 128, :]) for i in range(E * CAP // 128)],
            axis=1,
        )
        high = turned.astype(bf16)
        whi[...] = high
        wlo[...] = (turned - high.astype(f32)).astype(bf16)

    def gram_part():
        for dz in range(1, NZ):
            receive(gall.at[y, layer_of(-dz)], g1s.at[dz], g1r.at[dz], ffn(dz, 0))
        for dy in range(1, NY):
            send(gall.at[y], gall.at[y], g2s.at[dy], g2r.at[dy], ffn(0, dy))

    def gather_send(plan, ref, sems, key):
        step, block, (r0, n) = plan.msgs[key]
        view = ref.at[at(*block), pl.ds(r0, n)]
        i = plan.index[key]
        send(view, view, sems[0].at[i], sems[1].at[i], ffn(*step))

    def gather_receive(plan, ref, sems, key):
        step, _, (r0, n) = plan.msgs[key]
        view = ref.at[at(*plan.target(key)), pl.ds(r0, n)]
        i = plan.index[key]
        receive(view, sems[0].at[i], sems[1].at[i], ffn(*step))

    def reduce_send(plan, key):
        step, _, (r0, n) = plan.msgs[key]
        i = plan.index[key]
        send(
            vb.at[at(*plan.target(key)), pl.ds(r0, n)], rb.at[pl.ds(plan.offset[key], n)],
            rss.at[i], rsr.at[i], ffn(-step[0], -step[1]),
        )

    def reduce_receive(plan, key):
        step, block, (r0, n) = plan.msgs[key]
        i = plan.index[key]
        rows = pl.ds(plan.offset[key], n)
        receive(rb.at[rows], rss.at[i], rsr.at[i], ffn(-step[0], -step[1]))
        here = at(*block)
        vb[here, r0:r0 + n, :] = (
            vb[here, r0:r0 + n, :].astype(f32) + rb[rows, :].astype(f32)
        ).astype(bf16)

    def expand(dz, opening):
        if opening:
            for load in loads:
                load.wait()
        zz = layer_of(dz)
        lhs = jnp.concatenate([buf[zz * NY + i] for i in range(NY)], axis=1)
        for m in range(2):
            part = jnp.dot(lhs, w[m, zz], preferred_element_type=f32)
            acc[m] = part if opening else acc[m] + part

    def activate():
        gate, up = acc[0], acc[1]
        hid[...] = (gate / (1.0 + jnp.exp(-gate)) * up).astype(bf16)
        for load in late_loads:
            load.wait()

    def down(dz):
        zz = layer_of(dz)
        value = jnp.dot(hid[...], wd[zz], preferred_element_type=f32).astype(bf16)
        for i in range(NY):
            vb[zz * NY + i] = value[:, i * 128:(i + 1) * 128]

    for kind, first_arg, second_arg in SLOT_STEPS:
        if kind == "send" and first_arg == "gather":
            gather_send(SLOTS, buf, (ags, agr), second_arg)
        elif kind == "recv" and first_arg == "gather":
            gather_receive(SLOTS, buf, (ags, agr), second_arg)
        elif kind == "send":
            reduce_send(SLOTS, second_arg)
        elif kind == "recv":
            reduce_receive(SLOTS, second_arg)
        elif kind == "dot":
            expand(first_arg, second_arg)
        elif kind == "act":
            activate()
        elif kind == "down":
            down(first_arg)
        elif first_arg == "aux":
            aux_part()
        else:
            gram_part()

    for d in (4, 3, 5, 2, 6, 1, 7):
        send(
            vb.at[f, slot_rows(lax.rem(e + d, E))], rx.at[slot_rows(e)],
            ys.at[d], yr.at[d], peer(d),
        )
    rx[slot_rows(e), :] = vb[f, slot_rows(e), :]
    for dy in range(1, NY):
        receive(gall.at[col(-dy)], g2s.at[dy], g2r.at[dy], ffn(0, dy))
    for d in (1, 7, 2, 6, 3, 5, 4):
        receive(rx.at[slot_rows(lax.rem(e + E - d, E))], ys.at[d], yr.at[d], peer(d))
    mixture = jnp.dot(whi[...], rx[...], preferred_element_type=f32) + jnp.dot(
        wlo[...], rx[...], preferred_element_type=f32
    )
    layer_cols = tcol[...].astype(f32) + mixture
    lbuf[f] = jnp.transpose(layer_cols).astype(bf16)
    outs = []

    def contract(dz, opening):
        zz = layer_of(dz)
        blocks = pl.ds(zz * NY, NY)
        out = pltpu.make_async_copy(lbuf.at[blocks], layer_hbm.at[blocks], out_sem.at[len(outs)])
        out.start()
        outs.append(out)
        block = jnp.concatenate([lbuf[zz * NY + i] for i in range(NY)], axis=0)
        turned = (((0,), (0,)), ((), ()))
        gram_g = lax.dot_general(block, block, turned, preferred_element_type=f32)
        adp_g = lax.dot_general(block, ad[zz], turned, preferred_element_type=f32)
        gram[...] = gram_g if opening else gram[...] + gram_g
        adp[...] = adp_g if opening else adp[...] + adp_g

    for kind, first_arg, second_arg in LAYER_STEPS:
        if kind == "send":
            gather_send(LAYER, lbuf, (lgs, lgr), second_arg)
        elif kind == "recv":
            gather_receive(LAYER, lbuf, (lgs, lgr), second_arg)
        else:
            contract(first_arg, second_arg)

    whole_gram = jnp.concatenate(
        [gall[i % NY, i // NY] for i in range(NZ * NY)], axis=0
    )
    squared = jnp.sum(
        jnp.sum(gram[...] * whole_gram, axis=1, keepdims=True), axis=0, keepdims=True
    )
    limit = bound_ref[0]
    norm = jnp.sqrt(jnp.maximum(squared, 0.0))
    factor_ref[...] = jnp.broadcast_to(limit / jnp.maximum(norm, limit), factor_ref.shape)
    own_cols = layer_cols.astype(bf16).astype(f32)
    adapted_ref[...] = (own_cols + adp[...]).astype(bf16)
    for copy in sent:
        copy.wait_send()
    for out in outs:
        out.wait()


def grad_kernel(layer, up, factor, adapted, adapted_out, clipped_hbm, blocks, last_sem, out_sem):
    last = pltpu.make_async_copy(adapted, adapted_out, last_sem)
    last.start()
    stores = []
    scale = factor[0:1, 0:1]
    for g in range(NZ):
        part = jnp.concatenate([layer[g * NY + i] for i in range(NY)], axis=0)
        grad = jnp.dot(part, up[...], preferred_element_type=f32)
        blocks[g] = (grad * scale).astype(bf16)
        store = pltpu.make_async_copy(
            blocks.at[g], clipped_hbm.at[pl.ds(g * 512, 512), :], out_sem.at[g]
        )
        store.start()
        stores.append(store)
    last.wait()
    for store in stores:
        store.wait()


def per_device(tokens, routes, router, w_gate, w_up, w_down, adapter, upstream, bound):
    F, E = NZ * NY, 8
    R = E * CAP
    dma = pltpu.SemaphoreType.DMA
    vmem = pl.BlockSpec(memory_space=pltpu.VMEM)
    hbm = pl.BlockSpec(memory_space=pl.ANY)
    V = pltpu.VMEM
    n1, n2 = len(SLOTS.keys), len(LAYER.keys)
    scratch = [
        V((4, NZ * NY * 128), bf16), V((2, 128), jnp.int32), V((E, NZ * NY * 128), bf16),
        V((128, 128), bf16),
        V((2, NZ, 512, 384), bf16), V((NZ, 384, 512), bf16), V((NZ, 512, 128), bf16),
        V((NY, NZ, 4, 128), bf16), V((NY, NZ, 4, 128), bf16), V((NZ, NY, 4, 128), bf16),
        V((NY, NZ, 8, 128), f32), V((NY, NZ, 8, 128), f32), V((NZ, NY, 8, 128), f32),
        V((NY, NZ, 4, 128), f32), V((8, 128), f32),
        V((128, 128), bf16), V((R, 128), f32), V((128, R), bf16), V((128, R), bf16),
        V((E, CAP, 128), bf16), V((F, R, 128), bf16), V((2, R, 384), f32), V((R, 384), bf16),
        V((F, R, 128), bf16), V((SLOTS.total, 128), bf16), V((R, 128), bf16),
        V((F, 128, 128), bf16), V((128, 128), f32), V((128, 128), f32),
        dma((4,)), dma((NZ,)), dma((4, NZ)),
        dma((NY,)), dma((NY,)), dma((NZ,)), dma((NZ,)),
        dma((NY,)), dma((NY,)), dma((NZ,)), dma((NZ,)),
        dma((NZ,)), dma((NZ,)), dma((NY,)), dma((NY,)),
        dma((E,)), dma((E,)), dma((E,)), dma((E,)),
        dma((n1,)), dma((n1,)), dma((n1,)), dma((n1,)), dma((n2,)), dma((n2,)),
    ]
    layer, adapted, factor = pl.pallas_call(
        layer_kernel,
        out_shape=(
            jax.ShapeDtypeStruct((F, 128, 128), bf16),
            jax.ShapeDtypeStruct((128, 128), bf16),
            jax.ShapeDtypeStruct((8, 128), f32),
        ),
        in_specs=[hbm] * 8 + [pl.BlockSpec(memory_space=pltpu.SMEM)],
        out_specs=(hbm, vmem, vmem),
        scratch_shapes=scratch,
        compiler_params=pltpu.CompilerParams(
            collective_id=0, has_side_effects=True, vmem_limit_bytes=55_000_000
        ),
    )(
        *[pltpu.with_memory_space_constraint(a, pltpu.HBM) for a in (
            tokens[0], routes[0].T, router.T, w_gate[0], w_up[0], w_down[0], adapter[0],
            upstream[0],
        )],
        bound,
    )
    adapted, clipped = pl.pallas_call(
        grad_kernel,
        out_shape=(
            jax.ShapeDtypeStruct((128, 128), bf16),
            jax.ShapeDtypeStruct((F * 128, 128), bf16),
        ),
        in_specs=[vmem] * 4,
        out_specs=(hbm, hbm),
        scratch_shapes=[
            V((NZ, 512, 128), bf16), pltpu.SemaphoreType.DMA, dma((NZ,)),
        ],
        compiler_params=pltpu.CompilerParams(vmem_limit_bytes=8_000_000),
    )(layer, upstream[0], factor, adapted)
    return (adapted[None], clipped[None])


def solution(mesh):
    in_specs = (
        P("expert", "ffn", None),
        P("expert", None, None),
        P(),
        P("expert", None, "ffn"),
        P("expert", None, "ffn"),
        P("expert", "ffn", None),
        P("expert", None, "ffn"),
        P("expert", None, "ffn"),
        P("expert"),
    )
    out_specs = (P("expert", None, "ffn"), P("expert", None, "ffn"))
    return jax.shard_map(
        per_device, mesh=mesh, in_specs=in_specs, out_specs=out_specs, check_vma=False
    )
```

```python
import functools

import jax
import jax.numpy as jnp
from jax import lax
from jax.experimental import pallas as pl
from jax.experimental.pallas import tpu as pltpu
from jax.sharding import PartitionSpec as P

MESH = pl.DeviceIdType.MESH
NZ, NY = 8, 4
CAP = 48
bf16, f32 = jnp.bfloat16, jnp.float32


LATENCY, ROUTED, RATE = 2.0, 0.75, 46.6e3
RING, SKIP = {1: 0, 2: 1, 3: 2, 4: 3}, {1: 0, 2: 0, 3: 2, 4: 2}
HALFSKIP = {1: 0, 2: 0, 3: 2, 4: 3}
YRING, YDIRECT = {1: 0, 2: 1}, {1: 0, 2: 0}


class Plan:
    def __init__(self, base, rows, rows_a, za, ya, yb, zb):
        half_a = -(-rows_a // 32) * 16
        rows_b = rows - rows_a
        half_b = -(-rows_b // 32) * 16
        A = ((0, rows_a), (0, half_a), (half_a, rows_a - half_a))
        B = ((rows_a, rows_b), (rows_a, half_b), (rows_a + half_b, rows_b - half_b))
        self.msgs, self.deps = {}, {}

        def line(name, parents, part, move, needs):
            last = max(parents)
            for k in sorted(parents):
                for s in (1, -1):
                    j = parents[k]
                    rows_k = part[0] if k < last else part[1 if s > 0 else 2]
                    if rows_k[1] == 0:
                        continue
                    step, block = move(s, k, j)
                    self.msgs[name + (s, k)] = (step, block, (base + rows_k[0], rows_k[1]))
                    self.deps[name + (s, k)] = [name + (s, j)] if j else needs

        line(("Az",), za, A, lambda s, k, j: ((s * (k - j), 0), (-s * j, 0)), [])
        line(("By",), yb, B, lambda s, k, j: ((0, s * (k - j)), (0, -s * j)), [])
        for bz in (0, -1, 1, -2, 2, -3, 3, -4):
            needs = [] if bz == 0 else [("Az", -1 if bz > 0 else 1, abs(bz))]
            if abs(bz) == NZ // 2:
                needs = [("Az", 1, NZ // 2), ("Az", -1, NZ // 2)]
            line(("Ay", bz), ya, A, lambda s, k, j: ((0, s * (k - j)), (bz, -s * j)), needs)
        for by in (0, -1, 1, 2):
            needs = [] if by == 0 else [("By", -1 if by > 0 else 1, abs(by))]
            if abs(by) == NY // 2:
                needs = [("By", 1, NY // 2), ("By", -1, NY // 2)]
            line(("Bz", by), zb, B, lambda s, k, j: ((s * (k - j), 0), (-s * j, by)), needs)
        self.keys = list(self.msgs)
        self.index = {key: i for i, key in enumerate(self.keys)}
        self.users = {key: [u for u in self.keys if key in self.deps[u]] for key in self.keys}
        self.offset, self.total = {}, 0
        for key in self.keys:
            self.offset[key] = self.total
            self.total += self.msgs[key][2][1]

    def target(self, key):
        step, block, _ = self.msgs[key]
        return (block[0] - step[0], block[1] - step[1])

    def near(self, dz):
        return (dz + NZ // 2 - 1) % NZ - (NZ // 2 - 1)


def schedule(plans, starts, reduce, costs, throttle, extras=()):
    cost_dot, cost_act, cost_down, cost_add = costs
    far_first = (4, 3, -3, 2, -2, 1, -1, 0)
    keys = [(h, key) for h, plan in enumerate(plans) for key in plan.keys]
    place = {hk: i for i, hk in enumerate(keys)}
    deps = {(h, k): [(h, n) for n in plans[h].deps[k]] for h, k in keys}
    users = {(h, k): [(h, n) for n in plans[h].users[k]] for h, k in keys}
    goal = {(h, k): plans[h].near(plans[h].target(k)[0]) for h, k in keys}

    def shape(hk):
        step, _, (_, n) = plans[hk[0]].msgs[hk[1]]
        return (step[0] != 0, step[0] + step[1] > 0), abs(step[0] + step[1]), 0.03 + n * 256 / RATE

    def tails(after):
        found = {}

        def tail(hk):
            if hk not in found:
                _, hops, wire = shape(hk)
                found[hk] = LATENCY + hops * wire + max([tail(u) for u in after[hk]], default=0.0)
            return found[hk]

        for hk in keys:
            tail(hk)
        return found

    tail_of = {"gather": tails(users), "reduce": tails(deps)}
    before = {"gather": deps, "reduce": users}
    done = {"gather": set(), "reduce": set()}
    queued = {"gather": set(), "reduce": set()}
    groups = {dz: {hk for hk in keys if goal[hk] == dz} for dz in far_first}
    dots, acted, downs, ended = [], False, [], set()
    clock, links, flying, steps, extras, ready = 0.0, {}, [], [], list(extras), []
    while True:
        for mode in ("gather", "reduce"):
            for hk in keys:
                if hk not in queued[mode] and all(n in done[mode] for n in before[mode][hk]) and (
                    clock >= starts[hk[0]] if mode == "gather" else goal[hk] in downs
                ):
                    queued[mode].add(hk)
                    rank = tail_of[mode][hk] + (100.0 if mode == "gather" else 0.0)
                    ready.append((-rank, place[hk], mode, hk))
        ready.sort()
        for item in list(ready):
            _, _, mode, hk = item
            link, hops, wire = shape(hk)
            if mode == "reduce":
                link = (link[0], not link[1])
            if links.get(link, 0.0) - clock < throttle:
                ready.remove(item)
                clock += 0.035
                links[link] = max(clock, links.get(link, 0.0)) + hops * wire
                flying.append((links[link] + LATENCY + (hops - 1) * ROUTED, len(steps), mode, hk))
                steps.append(("send", mode, hk))
        flying.sort()
        if flying and flying[0][0] <= clock:
            _, _, mode, hk = flying.pop(0)
            clock += 0.035
            if mode == "reduce":
                clock += cost_add * shape(hk)[2]
            steps.append(("recv", mode, hk))
            done[mode].add(hk)
            h = hk[0]
            if mode == "reduce" and h not in ended and all(
                (h, k) in done["reduce"] for k in plans[h].keys
            ):
                ended.add(h)
                steps.append(("end", h, None))
            continue
        full = [dz for dz in reversed(far_first) if dz not in dots and groups[dz] <= done["gather"]]
        waiting = [start for start in starts if start > clock]
        if extras and extras[0][1] <= clock:
            name, _, cost = extras.pop(0)
            steps.append(("extra", name, None))
            clock += cost
        elif full:
            dots.append(full[0])
            steps.append(("dot", full[0], len(dots) == 1))
            clock += cost_dot
        elif reduce and len(dots) == NZ and not acted:
            acted = True
            steps.append(("act", None, None))
            clock += cost_act
        elif acted and len(downs) < NZ:
            downs.append(far_first[len(downs)])
            steps.append(("down", downs[-1], None))
            clock += cost_down
        elif flying or waiting:
            clock = max(clock, min([flight[0] for flight in flying[:1]] + waiting))
        elif ready:
            clock += 0.05
        else:
            return steps, clock


NEAR = ((0, 0), (0, 1), (1, 0), (1, 1), (3, 0), (3, 1), (2, 0), (2, 1))
PLACES = (range(0, 5), range(5, 8))
SLOTS = [
    Plan(0, 240, 240, HALFSKIP, YRING, YDIRECT, RING),
    Plan(240, 144, 0, HALFSKIP, YRING, YDIRECT, RING),
]
LAYER = [Plan(0, 128, 80, SKIP, YDIRECT, YRING, SKIP)]
SLOT_STEPS = schedule(
    SLOTS, (0.0, 1.3), True, (0.45, 0.2, 0.25, 0.05), 1.0, (("aux", 7.0, 1.0), ("gram", 15.0, 0.1))
)[0]
LAYER_STEPS = schedule(LAYER, (0.0,), False, (0.15, 0.0, 0.0, 0.0), 99.0)[0]


def layer_kernel(
    tok_hbm, routes_hbm, router_hbm, wg_hbm, wu_hbm, wd_hbm, ad_hbm, up_hbm, bound_ref,
    layer_hbm, adapted_ref, factor_ref,
    tok_ref, routes_ref, router_ref, up_ref, w, wd, ad, tok_s, tok_y, tok_z, aux_s, aux_y, aux_z, gall, lgp, tcol, pm, wsplit,
    pks, buf, acc, hid, vb, rb, rx, lbuf, sums,
    in_sem, out_sem, w_sem, a1s, a1r, a2s, a2r, b1s, b1r, b2s, b2r, g1s, g1r, g2s, g2r,
    xs, xr, ys, yr, ags, agr, rss, rsr, lgs, lgr,
):
    E = 8
    D = NZ * NY * 128
    e = lax.axis_index("expert")
    f = lax.axis_index("ffn")
    z, y = f // NY, lax.rem(f, NY)

    loads = []
    for g in range(NZ):
        rows = pl.ds(g * 512, 512)
        loads.append(pltpu.make_async_copy(wg_hbm.at[rows, :], w.at[0, g], w_sem.at[0, g]))
        loads.append(pltpu.make_async_copy(wu_hbm.at[rows, :], w.at[1, g], w_sem.at[1, g]))
    late_loads = []
    for g in range(NZ):
        late_loads.append(pltpu.make_async_copy(
            wd_hbm.at[:, pl.ds(g * 512, 512)], wd.at[g], w_sem.at[2, g]))
        late_loads.append(pltpu.make_async_copy(
            ad_hbm.at[pl.ds(g * 512, 512), :], ad.at[g], w_sem.at[3, g]))

    def at(dz, dy):
        return lax.rem(z + dz + NZ, NZ) * NY + lax.rem(y + dy + NY, NY)

    def ffn(dz, dy):
        return {"ffn": at(dz, dy)}

    def expert_at(dx, dc):
        core = lax.rem(e, 2)
        return lax.rem(e // 2 + dx, 4) * 2 + (1 - core if dc else core)

    def peer(dx, dc):
        return {"expert": expert_at(dx, dc)}

    def back(dx, dc):
        return NEAR.index(((4 - dx) % 4, dc))

    barrier = pltpu.get_barrier_semaphore()
    for dy in range(1, NY):
        pl.semaphore_signal(barrier, inc=1, device_id=ffn(0, dy), device_id_type=MESH)
    for dz in range(1, NZ):
        pl.semaphore_signal(barrier, inc=1, device_id=ffn(dz, 0), device_id_type=MESH)
    for d in NEAR[1:]:
        pl.semaphore_signal(barrier, inc=1, device_id=peer(*d), device_id_type=MESH)

    small = [
        pltpu.make_async_copy(src, dst, in_sem.at[i])
        for i, (src, dst) in enumerate((
            (tok_hbm, tok_ref), (up_hbm, up_ref), (router_hbm, router_ref),
            (routes_hbm, routes_ref),
        ))
    ]
    for load in small + loads:
        load.start()
    for load in small:
        load.wait()

    for i in range(NZ * NY):
        tok_s[i % NY, i // NY] = tok_ref[:, i * 128:(i + 1) * 128]
    tok_y[y] = tok_s[y]
    lgp[...] = jnp.zeros_like(lgp)
    lgp[0:4, 0:E] = lax.dot_general(
        tok_ref[...], router_ref[...], (((1,), (1,)), ((), ())), preferred_element_type=f32
    )
    own_logits = lgp[0:4, :]
    own_gram = lax.dot_general(
        up_ref[...], up_ref[...], (((1,), (1,)), ((), ())), preferred_element_type=f32
    )
    for i in range(NZ * NY):
        aux_s[i % NY, i // NY, 0:4, :] = own_logits
        aux_s[i % NY, i // NY, 4:8, :] = own_gram[4 * i:4 * i + 4, :]
    aux_y[y] = aux_s[y]

    first, second = routes_ref[0:1, :], routes_ref[1:2, :]
    expert_ids = lax.broadcasted_iota(jnp.int32, (E, 128), 0)
    hits = ((expert_ids == first) | (expert_ids == second)).astype(f32)
    before = (
        lax.broadcasted_iota(jnp.int32, (128, 128), 0)
        < lax.broadcasted_iota(jnp.int32, (128, 128), 1)
    ).astype(f32)
    rank = jnp.dot(hits.astype(bf16), before.astype(bf16), preferred_element_type=f32)
    slot = jnp.where(hits > 0.0, rank, -1.0)
    slot_ids = lax.broadcasted_iota(jnp.int32, (CAP, 128), 0).astype(f32)
    for i in range(E):
        pm[i * CAP:(i + 1) * CAP, :] = (slot_ids == slot[i:i + 1, :]).astype(f32)

    pl.semaphore_wait(barrier, NY - 1 + NZ - 1 + E - 1)

    sent = []

    def copy_of(src, dst, send_sem, recv_sem, device):
        return pltpu.make_async_remote_copy(
            src_ref=src, dst_ref=dst, send_sem=send_sem, recv_sem=recv_sem,
            device_id=device, device_id_type=MESH,
        )

    def send(src, dst, send_sem, recv_sem, device):
        copy = copy_of(src, dst, send_sem, recv_sem, device)
        copy.start()
        sent.append(copy)

    def receive(dst, send_sem, recv_sem, device):
        copy_of(dst, dst, send_sem, recv_sem, device).wait_recv()

    def col(dy):
        return lax.rem(y + dy + NY, NY)

    def layer_of(dz):
        return lax.rem(z + dz + NZ, NZ)

    for dy in (1, 3, 2):
        send(tok_s.at[col(dy)], tok_y.at[y], a1s.at[dy], a1r.at[dy], ffn(0, dy))
    for dy in (1, 3, 2):
        send(aux_s.at[col(dy)], aux_y.at[y], b1s.at[dy], b1r.at[dy], ffn(0, dy))
    for dy in (1, 3, 2):
        receive(tok_y.at[col(-dy)], a1s.at[dy], a1r.at[dy], ffn(0, dy))
    for dz in (4, 3, 5, 2, 6, 1, 7):
        send(tok_y.at[:, layer_of(dz)], tok_z.at[z], a2s.at[dz], a2r.at[dz], ffn(dz, 0))
    for i in range(NY):
        tok_z[z, i] = tok_y[i, z]
    for dy in (1, 3, 2):
        receive(aux_y.at[col(-dy)], b1s.at[dy], b1r.at[dy], ffn(0, dy))
    for dz in (1, 7, 2, 6, 3, 5, 4):
        receive(tok_z.at[layer_of(-dz)], a2s.at[dz], a2r.at[dz], ffn(dz, 0))
    own_tokens = jnp.concatenate(
        [tok_z[i // NY, i % NY].astype(f32) for i in range(NZ * NY)], axis=0
    ).astype(bf16)
    tcol[...] = own_tokens
    packed = jnp.dot(pm[...].astype(bf16), own_tokens, preferred_element_type=f32).astype(bf16)
    for i in range(E):
        pks[i] = packed[i * CAP:(i + 1) * CAP, :]

    def slot_rows(c):
        return pl.ds(pl.multiple_of(c * CAP, 16), CAP)

    def place_rows(p):
        return pl.ds(p * CAP, CAP)

    for d in NEAR[:0:-1]:
        p = back(*d)
        send(pks.at[expert_at(*d)], buf.at[f, place_rows(p)], xs.at[p], xr.at[p], peer(*d))
    buf[f, 0:CAP, :] = pks[e]
    for dz in range(1, NZ):
        send(aux_y.at[:, layer_of(dz)], aux_z.at[z], b2s.at[dz], b2r.at[dz], ffn(dz, 0))
    for i in range(NY):
        aux_z[z, i] = aux_y[i, z]
    for load in late_loads:
        load.start()

    def arrive(h):
        for p in PLACES[h]:
            if p:
                receive(buf.at[f, place_rows(p)], xs.at[p], xr.at[p], peer(*NEAR[p]))

    def aux_part():
        for dz in range(1, NZ):
            receive(aux_z.at[layer_of(-dz)], b2s.at[dz], b2r.at[dz], ffn(dz, 0))
        logit_rows = jnp.concatenate(
            [aux_z[i // NY, i % NY, 0:4, :] for i in range(NZ * NY)], axis=0
        )
        logits = jnp.transpose(logit_rows)[0:E, :]
        total = aux_z[0, 0, 4:8, :]
        for i in range(1, NZ * NY):
            total = total + aux_z[i // NY, i % NY, 4:8, :]
        gall[y, z] = total
        for dz in range(1, NZ):
            send(gall.at[y, z], gall.at[y, z], g1s.at[dz], g1r.at[dz], ffn(dz, 0))
        picked_first = jnp.sum(jnp.where(expert_ids == first, logits, 0.0), axis=0, keepdims=True)
        picked_second = jnp.sum(
            jnp.where(expert_ids == second, logits, 0.0), axis=0, keepdims=True
        )
        weight_first = 1.0 / (1.0 + jnp.exp(picked_second - picked_first))
        weights = jnp.where(expert_ids == first, weight_first, 1.0 - weight_first)
        weighted = jnp.concatenate(
            [pm[i * CAP:(i + 1) * CAP, :] * weights[i:i + 1, :] for i in range(E)], axis=0
        )
        turned = jnp.concatenate(
            [jnp.transpose(weighted[i * 128:(i + 1) * 128, :]) for i in range(E * CAP // 128)],
            axis=1,
        )
        high = turned.astype(bf16)
        wsplit[0:128, :] = high
        wsplit[128:256, :] = (turned - high.astype(f32)).astype(bf16)

    def gram_part():
        for dz in range(1, NZ):
            receive(gall.at[y, layer_of(-dz)], g1s.at[dz], g1r.at[dz], ffn(dz, 0))
        for dy in range(1, NY):
            send(gall.at[y], gall.at[y], g2s.at[dy], g2r.at[dy], ffn(0, dy))

    opened = set()

    def gather_send(plans, ref, sems, h, key):
        plan = plans[h]
        step, block, (r0, n) = plan.msgs[key]
        view = ref.at[at(*block), pl.ds(r0, n)]
        i = plan.index[key] + sum(len(q.keys) for q in plans[:h])
        send(view, view, sems[0].at[i], sems[1].at[i], ffn(*step))

    def gather_receive(plans, ref, sems, h, key):
        plan = plans[h]
        step, _, (r0, n) = plan.msgs[key]
        view = ref.at[at(*plan.target(key)), pl.ds(r0, n)]
        i = plan.index[key] + sum(len(q.keys) for q in plans[:h])
        receive(view, sems[0].at[i], sems[1].at[i], ffn(*step))

    def reduce_rows(h, key):
        plan = SLOTS[h]
        return pl.ds(plan.offset[key] + sum(q.total for q in SLOTS[:h]), plan.msgs[key][2][1])

    def reduce_send(h, key):
        plan = SLOTS[h]
        step, _, (r0, n) = plan.msgs[key]
        i = plan.index[key] + sum(len(q.keys) for q in SLOTS[:h])
        send(
            vb.at[at(*plan.target(key)), pl.ds(r0, n)], rb.at[reduce_rows(h, key)],
            rss.at[i], rsr.at[i], ffn(-step[0], -step[1]),
        )

    def reduce_receive(h, key):
        plan = SLOTS[h]
        step, block, (r0, n) = plan.msgs[key]
        i = plan.index[key] + sum(len(q.keys) for q in SLOTS[:h])
        rows = reduce_rows(h, key)
        receive(rb.at[rows], rss.at[i], rsr.at[i], ffn(-step[0], -step[1]))
        here = at(*block)
        vb[here, r0:r0 + n, :] = (
            vb[here, r0:r0 + n, :].astype(f32) + rb[rows, :].astype(f32)
        ).astype(bf16)

    def results(h):
        for p in reversed(PLACES[h]):
            if p:
                send(
                    vb.at[f, place_rows(p)], rx.at[slot_rows(e)], ys.at[p], yr.at[p],
                    peer(*NEAR[p]),
                )
            else:
                rx[slot_rows(e), :] = vb[f, 0:CAP, :]

    def expand(dz, opening):
        if opening:
            for load in loads:
                load.wait()
        zz = layer_of(dz)
        lhs = jnp.concatenate([buf[zz * NY + i] for i in range(NY)], axis=1)
        for m in range(2):
            part = jnp.dot(lhs, w[m, zz], preferred_element_type=f32)
            acc[m] = part if opening else acc[m] + part

    def activate():
        gate, up = acc[0], acc[1]
        hid[...] = (gate / (1.0 + jnp.exp(-gate)) * up).astype(bf16)
        for load in late_loads:
            load.wait()

    def down(dz):
        zz = layer_of(dz)
        value = jnp.dot(hid[...], wd[zz], preferred_element_type=f32).astype(bf16)
        for i in range(NY):
            vb[zz * NY + i] = value[:, i * 128:(i + 1) * 128]

    for kind, first_arg, second_arg in SLOT_STEPS:
        if kind == "send" and first_arg == "gather":
            if second_arg[0] not in opened:
                opened.add(second_arg[0])
                arrive(second_arg[0])
            gather_send(SLOTS, buf, (ags, agr), *second_arg)
        elif kind == "recv" and first_arg == "gather":
            gather_receive(SLOTS, buf, (ags, agr), *second_arg)
        elif kind == "send":
            reduce_send(*second_arg)
        elif kind == "recv":
            reduce_receive(*second_arg)
        elif kind == "dot":
            expand(first_arg, second_arg)
        elif kind == "act":
            activate()
        elif kind == "down":
            down(first_arg)
        elif kind == "end":
            results(first_arg)
        elif first_arg == "aux":
            aux_part()
        else:
            gram_part()

    for dy in range(1, NY):
        receive(gall.at[col(-dy)], g2s.at[dy], g2r.at[dy], ffn(0, dy))
    for d in NEAR[1:]:
        p = back(*d)
        receive(rx.at[slot_rows(expert_at(*d))], ys.at[p], yr.at[p], peer(*d))
    halves = jnp.dot(wsplit[...], rx[...], preferred_element_type=f32)
    mixture = halves[0:128, :] + halves[128:256, :]
    layer_cols = tcol[...].astype(f32) + mixture
    lbuf[f] = jnp.transpose(layer_cols).astype(bf16)
    outs = []

    def contract(dz, opening):
        zz = layer_of(dz)
        blocks = pl.ds(zz * NY, NY)
        out = pltpu.make_async_copy(lbuf.at[blocks], layer_hbm.at[blocks], out_sem.at[len(outs)])
        out.start()
        outs.append(out)
        block = jnp.concatenate([lbuf[zz * NY + i] for i in range(NY)], axis=0)
        both = lax.dot_general(
            block, jnp.concatenate([block, ad[zz]], axis=1), (((0,), (0,)), ((), ())),
            preferred_element_type=f32,
        )
        sums[...] = both if opening else sums[...] + both

    for kind, first_arg, second_arg in LAYER_STEPS:
        if kind == "send":
            gather_send(LAYER, lbuf, (lgs, lgr), *second_arg)
        elif kind == "recv":
            gather_receive(LAYER, lbuf, (lgs, lgr), *second_arg)
        else:
            contract(first_arg, second_arg)

    whole_gram = jnp.concatenate(
        [gall[i % NY, i // NY] for i in range(NZ * NY)], axis=0
    )
    squared = jnp.sum(
        jnp.sum(sums[:, 0:128] * whole_gram, axis=1, keepdims=True), axis=0, keepdims=True
    )
    limit = bound_ref[0]
    norm = jnp.sqrt(jnp.maximum(squared, 0.0))
    factor_ref[...] = jnp.broadcast_to(limit / jnp.maximum(norm, limit), factor_ref.shape)
    own_cols = layer_cols.astype(bf16).astype(f32)
    adapted_ref[...] = (own_cols + sums[:, 128:256]).astype(bf16)
    for copy in sent:
        copy.wait_send()
    for out in outs:
        out.wait()


def grad_kernel(
    layer, up, factor, adapted, adapted_out, clipped_hbm, blocks, last_sem, out_sem
):
    last = pltpu.make_async_copy(adapted, adapted_out, last_sem)
    last.start()
    stores = []
    scale = factor[0:1, 0:1]
    for g in range(NZ):
        part = jnp.concatenate([layer[g * NY + i] for i in range(NY)], axis=0)
        grad = jnp.dot(part, up[...], preferred_element_type=f32)
        blocks[g] = (grad * scale).astype(bf16)
        store = pltpu.make_async_copy(
            blocks.at[g], clipped_hbm.at[pl.ds(g * 512, 512), :], out_sem.at[g]
        )
        store.start()
        stores.append(store)
    last.wait()
    for store in stores:
        store.wait()


def per_device(tokens, routes, router, w_gate, w_up, w_down, adapter, upstream, bound):
    F, E = NZ * NY, 8
    R = E * CAP
    dma = pltpu.SemaphoreType.DMA
    vmem = pl.BlockSpec(memory_space=pltpu.VMEM)
    hbm = pl.BlockSpec(memory_space=pl.ANY)
    V = pltpu.VMEM
    n1, n2 = sum(len(p.keys) for p in SLOTS), len(LAYER[0].keys)
    scratch = [
        V((4, NZ * NY * 128), bf16), V((2, 128), jnp.int32), V((E, NZ * NY * 128), bf16),
        V((128, 128), bf16),
        V((2, NZ, 512, 384), bf16), V((NZ, 384, 512), bf16), V((NZ, 512, 128), bf16),
        V((NY, NZ, 4, 128), bf16), V((NY, NZ, 4, 128), bf16), V((NZ, NY, 4, 128), bf16),
        V((NY, NZ, 8, 128), f32), V((NY, NZ, 8, 128), f32), V((NZ, NY, 8, 128), f32),
        V((NY, NZ, 4, 128), f32), V((8, 128), f32),
        V((128, 128), bf16), V((R, 128), f32), V((256, R), bf16),
        V((E, CAP, 128), bf16), V((F, R, 128), bf16), V((2, R, 384), f32), V((R, 384), bf16),
        V((F, R, 128), bf16), V((sum(p.total for p in SLOTS), 128), bf16), V((R, 128), bf16),
        V((F, 128, 128), bf16), V((128, 256), f32),
        dma((4,)), dma((NZ,)), dma((4, NZ)),
        dma((NY,)), dma((NY,)), dma((NZ,)), dma((NZ,)),
        dma((NY,)), dma((NY,)), dma((NZ,)), dma((NZ,)),
        dma((NZ,)), dma((NZ,)), dma((NY,)), dma((NY,)),
        dma((E,)), dma((E,)), dma((E,)), dma((E,)),
        dma((n1,)), dma((n1,)), dma((n1,)), dma((n1,)), dma((n2,)), dma((n2,)),
    ]
    layer, adapted, factor = pl.pallas_call(
        layer_kernel,
        out_shape=(
            jax.ShapeDtypeStruct((F, 128, 128), bf16),
            jax.ShapeDtypeStruct((128, 128), bf16),
            jax.ShapeDtypeStruct((8, 128), f32),
        ),
        in_specs=[hbm] * 8 + [pl.BlockSpec(memory_space=pltpu.SMEM)],
        out_specs=(hbm, vmem, vmem),
        scratch_shapes=scratch,
        compiler_params=pltpu.CompilerParams(
            collective_id=0, has_side_effects=True, vmem_limit_bytes=55_000_000
        ),
    )(
        *[pltpu.with_memory_space_constraint(a, pltpu.HBM) for a in (
            tokens[0], routes[0].T, router.T, w_gate[0], w_up[0], w_down[0], adapter[0],
            upstream[0],
        )],
        bound,
    )
    adapted, clipped = pl.pallas_call(
        grad_kernel,
        out_shape=(
            jax.ShapeDtypeStruct((128, 128), bf16),
            jax.ShapeDtypeStruct((F * 128, 128), bf16),
        ),
        in_specs=[vmem] * 4,
        out_specs=(hbm, hbm),
        scratch_shapes=[
            V((NZ, 512, 128), bf16), pltpu.SemaphoreType.DMA, dma((NZ,)),
        ],
        compiler_params=pltpu.CompilerParams(vmem_limit_bytes=8_000_000),
    )(layer, upstream[0], factor, adapted)
    return (adapted[None], clipped[None])


def solution(mesh):
    in_specs = (
        P("expert", "ffn", None),
        P("expert", None, None),
        P(),
        P("expert", None, "ffn"),
        P("expert", None, "ffn"),
        P("expert", "ffn", None),
        P("expert", None, "ffn"),
        P("expert", None, "ffn"),
        P("expert"),
    )
    out_specs = (P("expert", None, "ffn"), P("expert", None, "ffn"))
    return jax.shard_map(
        per_device, mesh=mesh, in_specs=in_specs, out_specs=out_specs, check_vma=False
    )
```

```python
import functools

import jax
import jax.numpy as jnp
from jax import lax
from jax.experimental import pallas as pl
from jax.experimental.pallas import tpu as pltpu
from jax.sharding import PartitionSpec as P

MESH = pl.DeviceIdType.MESH
NZ, NY = 8, 4
CAP = 48
bf16, f32 = jnp.bfloat16, jnp.float32


LATENCY, ROUTED, RATE = 2.0, 0.75, 46.6e3
RING, SKIP = {1: 0, 2: 1, 3: 2, 4: 3}, {1: 0, 2: 0, 3: 2, 4: 2}
HALFSKIP = {1: 0, 2: 0, 3: 2, 4: 3}
YRING, YDIRECT = {1: 0, 2: 1}, {1: 0, 2: 0}


class Plan:
    def __init__(self, base, rows, rows_a, za, ya, yb, zb):
        half_a = -(-rows_a // 32) * 16
        rows_b = rows - rows_a
        half_b = -(-rows_b // 32) * 16
        A = ((0, rows_a), (0, half_a), (half_a, rows_a - half_a))
        B = ((rows_a, rows_b), (rows_a, half_b), (rows_a + half_b, rows_b - half_b))
        self.msgs, self.deps = {}, {}

        def line(name, parents, part, move, needs):
            last = max(parents)
            for k in sorted(parents):
                for s in (1, -1):
                    j = parents[k]
                    rows_k = part[0] if k < last else part[1 if s > 0 else 2]
                    if rows_k[1] == 0:
                        continue
                    step, block = move(s, k, j)
                    self.msgs[name + (s, k)] = (step, block, (base + rows_k[0], rows_k[1]))
                    self.deps[name + (s, k)] = [name + (s, j)] if j else needs

        line(("Az",), za, A, lambda s, k, j: ((s * (k - j), 0), (-s * j, 0)), [])
        line(("By",), yb, B, lambda s, k, j: ((0, s * (k - j)), (0, -s * j)), [])
        for bz in (0, -1, 1, -2, 2, -3, 3, -4):
            needs = [] if bz == 0 else [("Az", -1 if bz > 0 else 1, abs(bz))]
            if abs(bz) == NZ // 2:
                needs = [("Az", 1, NZ // 2), ("Az", -1, NZ // 2)]
            line(("Ay", bz), ya, A, lambda s, k, j: ((0, s * (k - j)), (bz, -s * j)), needs)
        for by in (0, -1, 1, 2):
            needs = [] if by == 0 else [("By", -1 if by > 0 else 1, abs(by))]
            if abs(by) == NY // 2:
                needs = [("By", 1, NY // 2), ("By", -1, NY // 2)]
            line(("Bz", by), zb, B, lambda s, k, j: ((s * (k - j), 0), (-s * j, by)), needs)
        self.keys = list(self.msgs)
        self.index = {key: i for i, key in enumerate(self.keys)}
        self.users = {key: [u for u in self.keys if key in self.deps[u]] for key in self.keys}
        self.offset, self.total = {}, 0
        for key in self.keys:
            self.offset[key] = self.total
            self.total += self.msgs[key][2][1]

    def target(self, key):
        step, block, _ = self.msgs[key]
        return (block[0] - step[0], block[1] - step[1])

    def near(self, dz):
        return (dz + NZ // 2 - 1) % NZ - (NZ // 2 - 1)


def schedule(plans, starts, reduce, costs, throttle, extras=()):
    cost_dot, cost_act, cost_down, cost_add = costs
    far_first = (4, 3, -3, 2, -2, 1, -1, 0)
    keys = [(h, key) for h, plan in enumerate(plans) for key in plan.keys]
    place = {hk: i for i, hk in enumerate(keys)}
    deps = {(h, k): [(h, n) for n in plans[h].deps[k]] for h, k in keys}
    users = {(h, k): [(h, n) for n in plans[h].users[k]] for h, k in keys}
    goal = {(h, k): plans[h].near(plans[h].target(k)[0]) for h, k in keys}

    def shape(hk):
        step, _, (_, n) = plans[hk[0]].msgs[hk[1]]
        return (step[0] != 0, step[0] + step[1] > 0), abs(step[0] + step[1]), 0.03 + n * 256 / RATE

    def tails(after):
        found = {}

        def tail(hk):
            if hk not in found:
                _, hops, wire = shape(hk)
                found[hk] = LATENCY + hops * wire + max([tail(u) for u in after[hk]], default=0.0)
            return found[hk]

        for hk in keys:
            tail(hk)
        return found

    tail_of = {"gather": tails(users), "reduce": tails(deps)}
    before = {"gather": deps, "reduce": users}
    done = {"gather": set(), "reduce": set()}
    queued = {"gather": set(), "reduce": set()}
    groups = {dz: {hk for hk in keys if goal[hk] == dz} for dz in far_first}
    dots, acted, downs, ended = [], False, [], set()
    clock, links, flying, steps, extras, ready = 0.0, {}, [], [], list(extras), []
    while True:
        for mode in ("gather", "reduce"):
            for hk in keys:
                if hk not in queued[mode] and all(n in done[mode] for n in before[mode][hk]) and (
                    clock >= starts[hk[0]] if mode == "gather" else goal[hk] in downs
                ):
                    queued[mode].add(hk)
                    rank = tail_of[mode][hk] + (100.0 if mode == "gather" else 0.0)
                    ready.append((-rank, place[hk], mode, hk))
        ready.sort()
        for item in list(ready):
            _, _, mode, hk = item
            link, hops, wire = shape(hk)
            if mode == "reduce":
                link = (link[0], not link[1])
            if links.get(link, 0.0) - clock < throttle:
                ready.remove(item)
                clock += 0.035
                links[link] = max(clock, links.get(link, 0.0)) + hops * wire
                flying.append((links[link] + LATENCY + (hops - 1) * ROUTED, len(steps), mode, hk))
                steps.append(("send", mode, hk))
        flying.sort()
        if flying and flying[0][0] <= clock:
            _, _, mode, hk = flying.pop(0)
            clock += 0.035
            if mode == "reduce":
                clock += cost_add * shape(hk)[2]
            steps.append(("recv", mode, hk))
            done[mode].add(hk)
            h = hk[0]
            if mode == "reduce" and h not in ended and all(
                (h, k) in done["reduce"] for k in plans[h].keys
            ):
                ended.add(h)
                steps.append(("end", h, None))
            continue
        full = [dz for dz in reversed(far_first) if dz not in dots and groups[dz] <= done["gather"]]
        waiting = [start for start in starts if start > clock]
        if extras and extras[0][1] <= clock:
            name, _, cost = extras.pop(0)
            steps.append(("extra", name, None))
            clock += cost
        elif full:
            dots.append(full[0])
            steps.append(("dot", full[0], len(dots) == 1))
            clock += cost_dot
        elif reduce and len(dots) == NZ and not acted:
            acted = True
            steps.append(("act", None, None))
            clock += cost_act
        elif acted and len(downs) < NZ:
            downs.append(far_first[len(downs)])
            steps.append(("down", downs[-1], None))
            clock += cost_down
        elif flying or waiting:
            clock = max(clock, min([flight[0] for flight in flying[:1]] + waiting))
        elif ready:
            clock += 0.05
        else:
            return steps, clock


NEAR = ((0, 0), (0, 1), (1, 0), (1, 1), (3, 0), (3, 1), (2, 0), (2, 1))
PLACES = (range(0, 5), range(5, 8))
SLOTS = [
    Plan(0, 240, 240, HALFSKIP, YRING, YDIRECT, RING),
    Plan(240, 144, 0, HALFSKIP, YRING, YDIRECT, RING),
]
LAYER = [Plan(0, 128, 64, SKIP, YDIRECT, YDIRECT, SKIP)]
SLOT_STEPS = schedule(
    SLOTS, (0.0, 1.3), True, (0.3, 0.15, 0.2, 0.03), 1.0, (("aux", 7.0, 1.0), ("gram", 15.0, 0.1))
)[0]
LAYER_STEPS = schedule(LAYER, (0.0,), False, (0.15, 0.0, 0.0, 0.0), 99.0)[0]


def layer_kernel(
    tok_hbm, routes_hbm, router_hbm, wg_hbm, wu_hbm, wd_hbm, ad_hbm, up_hbm, bound_ref,
    layer_hbm, adapted_ref, factor_ref,
    tok_ref, routes_ref, router_ref, up_ref, w, wd, ad, tok_s, tok_y, tok_z, aux_s, aux_y, aux_z, gall, lgp, tcol, pm, wsplit,
    pks, buf, acc, hid, vb, rb, rx, lbuf, sums,
    in_sem, out_sem, w_sem, a1s, a1r, a2s, a2r, b1s, b1r, b2s, b2r, g1s, g1r, g2s, g2r,
    xs, xr, ys, yr, ags, agr, rss, rsr, lgs, lgr,
):
    E = 8
    D = NZ * NY * 128
    e = lax.axis_index("expert")
    f = lax.axis_index("ffn")
    z, y = f // NY, lax.rem(f, NY)

    loads = []
    for g in range(NZ):
        rows = pl.ds(g * 512, 512)
        loads.append(pltpu.make_async_copy(wg_hbm.at[rows, :], w.at[0, g], w_sem.at[0, g]))
        loads.append(pltpu.make_async_copy(wu_hbm.at[rows, :], w.at[1, g], w_sem.at[1, g]))
    late_loads = []
    for g in range(NZ):
        late_loads.append(pltpu.make_async_copy(
            wd_hbm.at[:, pl.ds(g * 512, 512)], wd.at[g], w_sem.at[2, g]))
        late_loads.append(pltpu.make_async_copy(
            ad_hbm.at[pl.ds(g * 512, 512), :], ad.at[g], w_sem.at[3, g]))

    def at(dz, dy):
        return lax.rem(z + dz + NZ, NZ) * NY + lax.rem(y + dy + NY, NY)

    def ffn(dz, dy):
        return {"ffn": at(dz, dy)}

    def expert_at(dx, dc):
        core = lax.rem(e, 2)
        return lax.rem(e // 2 + dx, 4) * 2 + (1 - core if dc else core)

    def peer(dx, dc):
        return {"expert": expert_at(dx, dc)}

    def back(dx, dc):
        return NEAR.index(((4 - dx) % 4, dc))

    barrier = pltpu.get_barrier_semaphore()
    for dy in range(1, NY):
        pl.semaphore_signal(barrier, inc=1, device_id=ffn(0, dy), device_id_type=MESH)
    for dz in range(1, NZ):
        pl.semaphore_signal(barrier, inc=1, device_id=ffn(dz, 0), device_id_type=MESH)
    for d in NEAR[1:]:
        pl.semaphore_signal(barrier, inc=1, device_id=peer(*d), device_id_type=MESH)

    small = [
        pltpu.make_async_copy(src, dst, in_sem.at[i])
        for i, (src, dst) in enumerate((
            (tok_hbm, tok_ref), (up_hbm, up_ref), (router_hbm, router_ref),
            (routes_hbm, routes_ref),
        ))
    ]
    for load in small + loads:
        load.start()
    for load in small:
        load.wait()

    for i in range(NZ * NY):
        tok_s[i % NY, i // NY] = tok_ref[:, i * 128:(i + 1) * 128]
    tok_y[y] = tok_s[y]
    lgp[...] = jnp.zeros_like(lgp)
    lgp[0:4, 0:E] = lax.dot_general(
        tok_ref[...], router_ref[...], (((1,), (1,)), ((), ())), preferred_element_type=f32
    )
    own_logits = lgp[0:4, :]
    own_gram = lax.dot_general(
        up_ref[...], up_ref[...], (((1,), (1,)), ((), ())), preferred_element_type=f32
    )
    for i in range(NZ * NY):
        aux_s[i % NY, i // NY, 0:4, :] = own_logits
        aux_s[i % NY, i // NY, 4:8, :] = own_gram[4 * i:4 * i + 4, :]
    aux_y[y] = aux_s[y]

    first, second = routes_ref[0:1, :], routes_ref[1:2, :]
    expert_ids = lax.broadcasted_iota(jnp.int32, (E, 128), 0)
    hits = ((expert_ids == first) | (expert_ids == second)).astype(f32)
    before = (
        lax.broadcasted_iota(jnp.int32, (128, 128), 0)
        < lax.broadcasted_iota(jnp.int32, (128, 128), 1)
    ).astype(f32)
    rank = jnp.dot(hits.astype(bf16), before.astype(bf16), preferred_element_type=f32)
    slot = jnp.where(hits > 0.0, rank, -1.0)
    slot_ids = lax.broadcasted_iota(jnp.int32, (CAP, 128), 0).astype(f32)
    for i in range(E):
        pm[i * CAP:(i + 1) * CAP, :] = (slot_ids == slot[i:i + 1, :]).astype(f32)

    pl.semaphore_wait(barrier, NY - 1 + NZ - 1 + E - 1)

    sent = []

    def copy_of(src, dst, send_sem, recv_sem, device):
        return pltpu.make_async_remote_copy(
            src_ref=src, dst_ref=dst, send_sem=send_sem, recv_sem=recv_sem,
            device_id=device, device_id_type=MESH,
        )

    def send(src, dst, send_sem, recv_sem, device):
        copy = copy_of(src, dst, send_sem, recv_sem, device)
        copy.start()
        sent.append(copy)

    def receive(dst, send_sem, recv_sem, device):
        copy_of(dst, dst, send_sem, recv_sem, device).wait_recv()

    def col(dy):
        return lax.rem(y + dy + NY, NY)

    def layer_of(dz):
        return lax.rem(z + dz + NZ, NZ)

    for dy in (1, 3, 2):
        send(tok_s.at[col(dy)], tok_y.at[y], a1s.at[dy], a1r.at[dy], ffn(0, dy))
    for dy in (1, 3, 2):
        send(aux_s.at[col(dy)], aux_y.at[y], b1s.at[dy], b1r.at[dy], ffn(0, dy))
    for dy in (1, 3, 2):
        receive(tok_y.at[col(-dy)], a1s.at[dy], a1r.at[dy], ffn(0, dy))
    for dz in (4, 3, 5, 2, 6, 1, 7):
        send(tok_y.at[:, layer_of(dz)], tok_z.at[z], a2s.at[dz], a2r.at[dz], ffn(dz, 0))
    for i in range(NY):
        tok_z[z, i] = tok_y[i, z]
    for dy in (1, 3, 2):
        receive(aux_y.at[col(-dy)], b1s.at[dy], b1r.at[dy], ffn(0, dy))
    for dz in (1, 7, 2, 6, 3, 5, 4):
        receive(tok_z.at[layer_of(-dz)], a2s.at[dz], a2r.at[dz], ffn(dz, 0))
    own_tokens = jnp.concatenate(
        [tok_z[i // NY, i % NY].astype(f32) for i in range(NZ * NY)], axis=0
    ).astype(bf16)
    tcol[...] = own_tokens
    packed = jnp.dot(pm[...].astype(bf16), own_tokens, preferred_element_type=f32).astype(bf16)
    for i in range(E):
        pks[i] = packed[i * CAP:(i + 1) * CAP, :]

    def slot_rows(c):
        return pl.ds(pl.multiple_of(c * CAP, 16), CAP)

    def place_rows(p):
        return pl.ds(p * CAP, CAP)

    for d in NEAR[:0:-1]:
        p = back(*d)
        send(pks.at[expert_at(*d)], buf.at[f, place_rows(p)], xs.at[p], xr.at[p], peer(*d))
    buf[f, 0:CAP, :] = pks[e]
    for dz in range(1, NZ):
        send(aux_y.at[:, layer_of(dz)], aux_z.at[z], b2s.at[dz], b2r.at[dz], ffn(dz, 0))
    for i in range(NY):
        aux_z[z, i] = aux_y[i, z]
    for load in late_loads:
        load.start()

    def arrive(h):
        for p in PLACES[h]:
            if p:
                receive(buf.at[f, place_rows(p)], xs.at[p], xr.at[p], peer(*NEAR[p]))

    def aux_part():
        for dz in range(1, NZ):
            receive(aux_z.at[layer_of(-dz)], b2s.at[dz], b2r.at[dz], ffn(dz, 0))
        logit_rows = jnp.concatenate(
            [aux_z[i // NY, i % NY, 0:4, :] for i in range(NZ * NY)], axis=0
        )
        logits = jnp.transpose(logit_rows)[0:E, :]
        total = aux_z[0, 0, 4:8, :]
        for i in range(1, NZ * NY):
            total = total + aux_z[i // NY, i % NY, 4:8, :]
        gall[y, z] = total
        for dz in range(1, NZ):
            send(gall.at[y, z], gall.at[y, z], g1s.at[dz], g1r.at[dz], ffn(dz, 0))
        picked_first = jnp.sum(jnp.where(expert_ids == first, logits, 0.0), axis=0, keepdims=True)
        picked_second = jnp.sum(
            jnp.where(expert_ids == second, logits, 0.0), axis=0, keepdims=True
        )
        weight_first = 1.0 / (1.0 + jnp.exp(picked_second - picked_first))
        weights = jnp.where(expert_ids == first, weight_first, 1.0 - weight_first)
        weighted = jnp.concatenate(
            [pm[i * CAP:(i + 1) * CAP, :] * weights[i:i + 1, :] for i in range(E)], axis=0
        )
        turned = jnp.concatenate(
            [jnp.transpose(weighted[i * 128:(i + 1) * 128, :]) for i in range(E * CAP // 128)],
            axis=1,
        )
        high = turned.astype(bf16)
        wsplit[0:128, :] = high
        wsplit[128:256, :] = (turned - high.astype(f32)).astype(bf16)

    def gram_part():
        for dz in range(1, NZ):
            receive(gall.at[y, layer_of(-dz)], g1s.at[dz], g1r.at[dz], ffn(dz, 0))
        for dy in range(1, NY):
            send(gall.at[y], gall.at[y], g2s.at[dy], g2r.at[dy], ffn(0, dy))

    opened = set()

    def gather_send(plans, ref, sems, h, key):
        plan = plans[h]
        step, block, (r0, n) = plan.msgs[key]
        view = ref.at[at(*block), pl.ds(r0, n)]
        i = plan.index[key] + sum(len(q.keys) for q in plans[:h])
        send(view, view, sems[0].at[i], sems[1].at[i], ffn(*step))

    def gather_receive(plans, ref, sems, h, key):
        plan = plans[h]
        step, _, (r0, n) = plan.msgs[key]
        view = ref.at[at(*plan.target(key)), pl.ds(r0, n)]
        i = plan.index[key] + sum(len(q.keys) for q in plans[:h])
        receive(view, sems[0].at[i], sems[1].at[i], ffn(*step))

    def reduce_rows(h, key):
        plan = SLOTS[h]
        return pl.ds(plan.offset[key] + sum(q.total for q in SLOTS[:h]), plan.msgs[key][2][1])

    def reduce_send(h, key):
        plan = SLOTS[h]
        step, _, (r0, n) = plan.msgs[key]
        i = plan.index[key] + sum(len(q.keys) for q in SLOTS[:h])
        send(
            vb.at[at(*plan.target(key)), pl.ds(r0, n)], rb.at[reduce_rows(h, key)],
            rss.at[i], rsr.at[i], ffn(-step[0], -step[1]),
        )

    def reduce_receive(h, key):
        plan = SLOTS[h]
        step, block, (r0, n) = plan.msgs[key]
        i = plan.index[key] + sum(len(q.keys) for q in SLOTS[:h])
        rows = reduce_rows(h, key)
        receive(rb.at[rows], rss.at[i], rsr.at[i], ffn(-step[0], -step[1]))
        here = at(*block)
        vb[here, r0:r0 + n, :] = (
            vb[here, r0:r0 + n, :].astype(f32) + rb[rows, :].astype(f32)
        ).astype(bf16)

    def results(h):
        for p in reversed(PLACES[h]):
            if p:
                send(
                    vb.at[f, place_rows(p)], rx.at[slot_rows(e)], ys.at[p], yr.at[p],
                    peer(*NEAR[p]),
                )
            else:
                rx[slot_rows(e), :] = vb[f, 0:CAP, :]

    def expand(dz, opening):
        if opening:
            for load in loads:
                load.wait()
        zz = layer_of(dz)
        lhs = jnp.concatenate([buf[zz * NY + i] for i in range(NY)], axis=1)
        for m in range(2):
            part = jnp.dot(lhs, w[m, zz], preferred_element_type=f32)
            acc[m] = part if opening else acc[m] + part

    def activate():
        gate, up = acc[0], acc[1]
        hid[...] = (gate / (1.0 + jnp.exp(-gate)) * up).astype(bf16)
        for load in late_loads:
            load.wait()

    def down(dz):
        zz = layer_of(dz)
        value = jnp.dot(hid[...], wd[zz], preferred_element_type=f32).astype(bf16)
        for i in range(NY):
            vb[zz * NY + i] = value[:, i * 128:(i + 1) * 128]

    for kind, first_arg, second_arg in SLOT_STEPS:
        if kind == "send" and first_arg == "gather":
            if second_arg[0] not in opened:
                opened.add(second_arg[0])
                arrive(second_arg[0])
            gather_send(SLOTS, buf, (ags, agr), *second_arg)
        elif kind == "recv" and first_arg == "gather":
            gather_receive(SLOTS, buf, (ags, agr), *second_arg)
        elif kind == "send":
            reduce_send(*second_arg)
        elif kind == "recv":
            reduce_receive(*second_arg)
        elif kind == "dot":
            expand(first_arg, second_arg)
        elif kind == "act":
            activate()
        elif kind == "down":
            down(first_arg)
        elif kind == "end":
            results(first_arg)
        elif first_arg == "aux":
            aux_part()
        else:
            gram_part()

    for dy in range(1, NY):
        receive(gall.at[col(-dy)], g2s.at[dy], g2r.at[dy], ffn(0, dy))
    for d in NEAR[1:]:
        p = back(*d)
        receive(rx.at[slot_rows(expert_at(*d))], ys.at[p], yr.at[p], peer(*d))
    halves = jnp.dot(wsplit[...], rx[...], preferred_element_type=f32)
    mixture = halves[0:128, :] + halves[128:256, :]
    layer_cols = tcol[...].astype(f32) + mixture
    lbuf[f] = jnp.transpose(layer_cols).astype(bf16)
    outs = []

    def contract(dz, opening):
        zz = layer_of(dz)
        blocks = pl.ds(zz * NY, NY)
        out = pltpu.make_async_copy(lbuf.at[blocks], layer_hbm.at[blocks], out_sem.at[len(outs)])
        out.start()
        outs.append(out)
        block = jnp.concatenate([lbuf[zz * NY + i] for i in range(NY)], axis=0)
        both = lax.dot_general(
            block, jnp.concatenate([block, ad[zz]], axis=1), (((0,), (0,)), ((), ())),
            preferred_element_type=f32,
        )
        sums[...] = both if opening else sums[...] + both

    for kind, first_arg, second_arg in LAYER_STEPS:
        if kind == "send":
            gather_send(LAYER, lbuf, (lgs, lgr), *second_arg)
        elif kind == "recv":
            gather_receive(LAYER, lbuf, (lgs, lgr), *second_arg)
        else:
            contract(first_arg, second_arg)

    whole_gram = jnp.concatenate(
        [gall[i % NY, i // NY] for i in range(NZ * NY)], axis=0
    )
    squared = jnp.sum(
        jnp.sum(sums[:, 0:128] * whole_gram, axis=1, keepdims=True), axis=0, keepdims=True
    )
    limit = bound_ref[0]
    norm = jnp.sqrt(jnp.maximum(squared, 0.0))
    factor_ref[...] = jnp.broadcast_to(limit / jnp.maximum(norm, limit), factor_ref.shape)
    own_cols = layer_cols.astype(bf16).astype(f32)
    adapted_ref[...] = (own_cols + sums[:, 128:256]).astype(bf16)
    for copy in sent:
        copy.wait_send()
    for out in outs:
        out.wait()


def grad_kernel(
    layer, up, factor, adapted, adapted_out, clipped_hbm, blocks, last_sem, out_sem
):
    last = pltpu.make_async_copy(adapted, adapted_out, last_sem)
    last.start()
    stores = []
    scale = factor[0:1, 0:1]
    for g in range(NZ):
        part = jnp.concatenate([layer[g * NY + i] for i in range(NY)], axis=0)
        grad = jnp.dot(part, up[...], preferred_element_type=f32)
        blocks[g] = (grad * scale).astype(bf16)
        store = pltpu.make_async_copy(
            blocks.at[g], clipped_hbm.at[pl.ds(g * 512, 512), :], out_sem.at[g]
        )
        store.start()
        stores.append(store)
    last.wait()
    for store in stores:
        store.wait()


def per_device(tokens, routes, router, w_gate, w_up, w_down, adapter, upstream, bound):
    F, E = NZ * NY, 8
    R = E * CAP
    dma = pltpu.SemaphoreType.DMA
    vmem = pl.BlockSpec(memory_space=pltpu.VMEM)
    hbm = pl.BlockSpec(memory_space=pl.ANY)
    V = pltpu.VMEM
    n1, n2 = sum(len(p.keys) for p in SLOTS), len(LAYER[0].keys)
    scratch = [
        V((4, NZ * NY * 128), bf16), V((2, 128), jnp.int32), V((E, NZ * NY * 128), bf16),
        V((128, 128), bf16),
        V((2, NZ, 512, 384), bf16), V((NZ, 384, 512), bf16), V((NZ, 512, 128), bf16),
        V((NY, NZ, 4, 128), bf16), V((NY, NZ, 4, 128), bf16), V((NZ, NY, 4, 128), bf16),
        V((NY, NZ, 8, 128), f32), V((NY, NZ, 8, 128), f32), V((NZ, NY, 8, 128), f32),
        V((NY, NZ, 4, 128), f32), V((8, 128), f32),
        V((128, 128), bf16), V((R, 128), f32), V((256, R), bf16),
        V((E, CAP, 128), bf16), V((F, R, 128), bf16), V((2, R, 384), f32), V((R, 384), bf16),
        V((F, R, 128), bf16), V((sum(p.total for p in SLOTS), 128), bf16), V((R, 128), bf16),
        V((F, 128, 128), bf16), V((128, 256), f32),
        dma((4,)), dma((NZ,)), dma((4, NZ)),
        dma((NY,)), dma((NY,)), dma((NZ,)), dma((NZ,)),
        dma((NY,)), dma((NY,)), dma((NZ,)), dma((NZ,)),
        dma((NZ,)), dma((NZ,)), dma((NY,)), dma((NY,)),
        dma((E,)), dma((E,)), dma((E,)), dma((E,)),
        dma((n1,)), dma((n1,)), dma((n1,)), dma((n1,)), dma((n2,)), dma((n2,)),
    ]
    layer, adapted, factor = pl.pallas_call(
        layer_kernel,
        out_shape=(
            jax.ShapeDtypeStruct((F, 128, 128), bf16),
            jax.ShapeDtypeStruct((128, 128), bf16),
            jax.ShapeDtypeStruct((8, 128), f32),
        ),
        in_specs=[hbm] * 8 + [pl.BlockSpec(memory_space=pltpu.SMEM)],
        out_specs=(hbm, vmem, vmem),
        scratch_shapes=scratch,
        compiler_params=pltpu.CompilerParams(
            collective_id=0, has_side_effects=True, vmem_limit_bytes=55_000_000
        ),
    )(
        *[pltpu.with_memory_space_constraint(a, pltpu.HBM) for a in (
            tokens[0], routes[0].T, router.T, w_gate[0], w_up[0], w_down[0], adapter[0],
            upstream[0],
        )],
        bound,
    )
    adapted, clipped = pl.pallas_call(
        grad_kernel,
        out_shape=(
            jax.ShapeDtypeStruct((128, 128), bf16),
            jax.ShapeDtypeStruct((F * 128, 128), bf16),
        ),
        in_specs=[vmem] * 4,
        out_specs=(hbm, hbm),
        scratch_shapes=[
            V((NZ, 512, 128), bf16), pltpu.SemaphoreType.DMA, dma((NZ,)),
        ],
        compiler_params=pltpu.CompilerParams(vmem_limit_bytes=8_000_000),
    )(layer, upstream[0], factor, adapted)
    return (adapted[None], clipped[None])


def solution(mesh):
    in_specs = (
        P("expert", "ffn", None),
        P("expert", None, None),
        P(),
        P("expert", None, "ffn"),
        P("expert", None, "ffn"),
        P("expert", "ffn", None),
        P("expert", None, "ffn"),
        P("expert", None, "ffn"),
        P("expert"),
    )
    out_specs = (P("expert", None, "ffn"), P("expert", None, "ffn"))
    return jax.shard_map(
        per_device, mesh=mesh, in_specs=in_specs, out_specs=out_specs, check_vma=False
    )
```
